128 devices in a mesh: data: 128 (over z, y, x, core).
Axes of the slice: x: 4, y: 4, z: 4, core: 2. Of those that a mesh axis runs over, the one named last changes fastest.
Arguments:
- act_in: bfloat16 [131072, 768], P('data')
- grad_out: bfloat16 [131072, 768], P('data')
- w_up: bfloat16 [2, 768, 3072], replicated
- w_down: bfloat16 [2, 3072, 768], replicated
- master_up: float32 [2, 768, 3072], P(None, 'data')
- master_down: float32 [2, 3072, 768], P(None, 'data')
- exp_avg_up: float32 [2, 768, 3072], P(None, 'data')
- exp_avg_down: float32 [2, 3072, 768], P(None, 'data')
- exp_sq_up: float32 [2, 768, 3072], P(None, 'data')
- exp_sq_down: float32 [2, 3072, 768], P(None, 'data')
- learn_rate: float32 [], replicated
- clip_norm: float32 [], replicated
Outputs:
- output 1: bfloat16 [2, 768, 3072], replicated
- output 2: bfloat16 [2, 3072, 768], replicated
- output 3: float32 [2, 768, 3072], P(None, 'data')
- output 4: float32 [2, 3072, 768], P(None, 'data')
- output 5: float32 [2, 768, 3072], P(None, 'data')
- output 6: float32 [2, 3072, 768], P(None, 'data')
- output 7: float32 [2, 768, 3072], P(None, 'data')
- output 8: float32 [2, 3072, 768], P(None, 'data')
- output 9: float32 [], replicated
All inputs are finite; a program needn't handle non-finite values.
Results may differ from the reference program's by a relative error of at most 0.00398.
Values are sent between devices in bfloat16 or wider.
A program may use at most 1 GiB of HBM per device.

```python
import jax
import jax.numpy as jnp
from jax import lax

D = 768
FF = 3072
TOKENS_DEV = 1024
GROUP = 128
STEP = 10

BETA_ONE = 0.9
BETA_TWO = 0.95
ADAM_EPS = 1e-8
NORM_EPS = 1e-6
INV_SQRT_TWO = 0.7071067811865476
INV_SQRT_TWO_PI = 0.3989422804014327


def gelu_parts(pre_act):
    normal_cdf = 0.5 * (1.0 + lax.erf(pre_act * INV_SQRT_TWO))
    normal_pdf = jnp.exp(-0.5 * pre_act * pre_act) * INV_SQRT_TWO_PI
    return pre_act * normal_cdf, normal_cdf + pre_act * normal_pdf


def block_grads(act_blk, out_blk, w_up, w_down):
    z_one = jnp.dot(act_blk, w_up[0], preferred_element_type=jnp.float32)
    gelu_one, slope_one = gelu_parts(z_one)
    act_one = gelu_one.astype(jnp.bfloat16)
    hidden = jnp.dot(act_one, w_down[0], preferred_element_type=jnp.float32).astype(jnp.bfloat16)
    z_three = jnp.dot(hidden, w_up[1], preferred_element_type=jnp.float32)
    gelu_three, slope_three = gelu_parts(z_three)
    act_three = gelu_three.astype(jnp.bfloat16)
    g_four = jnp.dot(act_three.T, out_blk, preferred_element_type=jnp.float32)
    dz_three = (jnp.dot(out_blk, w_down[1].T, preferred_element_type=jnp.float32) * slope_three).astype(jnp.bfloat16)
    g_three = jnp.dot(hidden.T, dz_three, preferred_element_type=jnp.float32)
    d_hidden = jnp.dot(dz_three, w_up[1].T, preferred_element_type=jnp.float32).astype(jnp.bfloat16)
    g_two = jnp.dot(act_one.T, d_hidden, preferred_element_type=jnp.float32)
    dz_one = (jnp.dot(d_hidden, w_down[0].T, preferred_element_type=jnp.float32) * slope_one).astype(jnp.bfloat16)
    g_one = jnp.dot(act_blk.T, dz_one, preferred_element_type=jnp.float32)
    return jnp.stack([g_one, g_three]), jnp.stack([g_two, g_four])


def full_grads(act_in, grad_out, w_up, w_down):
    act_blocks = act_in.reshape(GROUP, TOKENS_DEV, D)
    out_blocks = grad_out.reshape(GROUP, TOKENS_DEV, D)

    def add_block(carry_sums, blocks):
        grad_up, grad_down = block_grads(blocks[0], blocks[1], w_up, w_down)
        return (carry_sums[0] + grad_up, carry_sums[1] + grad_down), None

    start_sums = (jnp.zeros((2, D, FF), jnp.float32), jnp.zeros((2, FF, D), jnp.float32))
    final_sums = lax.scan(add_block, start_sums, (act_blocks, out_blocks))[0]
    return final_sums[0] / GROUP, final_sums[1] / GROUP


def lamb_update(master, exp_avg, exp_sq, grad, clip_scale, learn_rate):
    bias_one = 1.0 - BETA_ONE ** STEP
    bias_two = 1.0 - BETA_TWO ** STEP
    avg_new = BETA_ONE * exp_avg + (1.0 - BETA_ONE) * clip_scale * grad
    sq_new = BETA_TWO * exp_sq + (1.0 - BETA_TWO) * (clip_scale * clip_scale) * (grad * grad)
    direction = (avg_new / bias_one) / (jnp.sqrt(sq_new / bias_two) + ADAM_EPS)
    master_norm = jnp.sqrt(jnp.sum(master * master, axis=(1, 2), keepdims=True))
    dir_norm = jnp.sqrt(jnp.sum(direction * direction, axis=(1, 2), keepdims=True))
    master_new = master - learn_rate * (master_norm / dir_norm) * direction
    return master_new, avg_new, sq_new


def row_profile(key, row_count, spread):
    walk = jnp.cumsum(jax.random.normal(key, (row_count,), jnp.float32)) / (row_count ** 0.5)
    return jnp.exp(spread * (walk - jnp.mean(walk)))


def setup_inputs(seed: int = 0) -> dict:
    keys = jax.random.split(jax.random.key(seed), 24)
    row_total = TOKENS_DEV * GROUP
    init_scale = D ** -0.5
    out_scale = (GROUP / TOKENS_DEV) ** 0.5
    act_in = jax.random.normal(keys[0], (row_total, D), jnp.float32).astype(jnp.bfloat16)
    grad_out = (jax.random.normal(keys[1], (row_total, D), jnp.float32) * out_scale).astype(jnp.bfloat16)
    prof_up = jnp.stack([row_profile(keys[2], D, 0.7), row_profile(keys[3], D, 0.7)])[:, :, None]
    prof_down = jnp.stack([row_profile(keys[4], FF, 0.7), row_profile(keys[5], FF, 0.7)])[:, :, None]
    base_up = jax.random.normal(keys[6], (2, D, FF), jnp.float32) * init_scale * prof_up
    base_down = jax.random.normal(keys[7], (2, FF, D), jnp.float32) * init_scale * prof_down
    w_up = base_up.astype(jnp.bfloat16)
    w_down = base_down.astype(jnp.bfloat16)
    master_up = base_up + 0.02 * init_scale * prof_up * jax.random.normal(keys[8], (2, D, FF), jnp.float32)
    master_down = base_down + 0.02 * init_scale * prof_down * jax.random.normal(keys[9], (2, FF, D), jnp.float32)
    grad_up, grad_down = full_grads(act_in, grad_out, w_up, w_down)
    grad_norm = jnp.sqrt(jnp.sum(grad_up * grad_up) + jnp.sum(grad_down * grad_down))
    clip_norm = jax.random.uniform(keys[10], (), jnp.float32, 0.3, 0.7) * grad_norm
    clip_scale = clip_norm / (grad_norm + NORM_EPS)
    step_up = clip_scale * jnp.sqrt(jnp.mean(grad_up * grad_up, axis=(1, 2), keepdims=True))
    step_down = clip_scale * jnp.sqrt(jnp.mean(grad_down * grad_down, axis=(1, 2), keepdims=True))
    exp_avg_up = 0.1 * step_up * jax.random.normal(keys[11], (2, D, FF), jnp.float32)
    exp_avg_down = 0.1 * step_down * jax.random.normal(keys[12], (2, FF, D), jnp.float32)
    sq_prof_up = jnp.stack([row_profile(keys[13], D, 1.5), row_profile(keys[14], D, 1.5)])[:, :, None]
    sq_prof_down = jnp.stack([row_profile(keys[15], FF, 1.5), row_profile(keys[16], FF, 1.5)])[:, :, None]
    exp_sq_up = 0.05 * step_up * step_up * sq_prof_up * jax.random.uniform(keys[17], (2, D, FF), jnp.float32, 0.5, 1.5)
    exp_sq_down = 0.05 * step_down * step_down * sq_prof_down * jax.random.uniform(keys[18], (2, FF, D), jnp.float32, 0.5, 1.5)
    learn_rate = jax.random.uniform(keys[19], (), jnp.float32, 0.08, 0.16)
    return {"act_in": act_in, "grad_out": grad_out, "w_up": w_up, "w_down": w_down, "master_up": master_up, "master_down": master_down, "exp_avg_up": exp_avg_up, "exp_avg_down": exp_avg_down, "exp_sq_up": exp_sq_up, "exp_sq_down": exp_sq_down, "learn_rate": learn_rate, "clip_norm": clip_norm}


def reference(act_in, grad_out, w_up, w_down, master_up, master_down, exp_avg_up, exp_avg_down, exp_sq_up, exp_sq_down, learn_rate, clip_norm):
    grad_up, grad_down = full_grads(act_in, grad_out, w_up, w_down)
    grad_norm = jnp.sqrt(jnp.sum(grad_up * grad_up) + jnp.sum(grad_down * grad_down))
    clip_scale = jnp.minimum(1.0, clip_norm / (grad_norm + NORM_EPS))
    master_up_out, avg_up, sq_up = lamb_update(master_up, exp_avg_up, exp_sq_up, grad_up, clip_scale, learn_rate)
    master_down_out, avg_down, sq_down = lamb_update(master_down, exp_avg_down, exp_sq_down, grad_down, clip_scale, learn_rate)
    return (master_up_out.astype(jnp.bfloat16), master_down_out.astype(jnp.bfloat16), master_up_out, master_down_out, avg_up, avg_down, sq_up, sq_down, grad_norm)
```

```python
import functools
import math

import jax
import jax.numpy as jnp
from jax import lax
from jax.experimental import pallas as pl
from jax.experimental.pallas import tpu as pltpu
from jax.sharding import PartitionSpec as P

STEP = 10
BETA_ONE = 0.9
BETA_TWO = 0.95
ADAM_EPS = 1e-8
NORM_EPS = 1e-6
INV_SQRT_TWO = 0.7071067811865476
INV_SQRT_TWO_PI = 0.3989422804014327

MESH = pl.DeviceIdType.MESH
F32 = jnp.float32
BF16 = jnp.bfloat16


def gelu_parts(pre_act):
    normal_cdf = 0.5 * (1.0 + lax.erf(pre_act * INV_SQRT_TWO))
    normal_pdf = jnp.exp(-0.5 * pre_act * pre_act) * INV_SQRT_TWO_PI
    return pre_act * normal_cdf, normal_cdf + pre_act * normal_pdf


def local_grads(act_in, grad_out, w_up, w_down):
    z_one = jnp.einsum("td,df->tf", act_in, w_up[0], preferred_element_type=jnp.float32)
    gelu_one, slope_one = gelu_parts(z_one)
    act_one = gelu_one.astype(jnp.bfloat16)
    hidden = jnp.einsum("tf,fd->td", act_one, w_down[0], preferred_element_type=jnp.float32).astype(jnp.bfloat16)
    z_three = jnp.einsum("td,df->tf", hidden, w_up[1], preferred_element_type=jnp.float32)
    gelu_three, slope_three = gelu_parts(z_three)
    act_three = gelu_three.astype(jnp.bfloat16)
    g_four = jnp.einsum("tf,td->fd", act_three, grad_out, preferred_element_type=jnp.float32)
    dz_three = (jnp.einsum("td,fd->tf", grad_out, w_down[1], preferred_element_type=jnp.float32) * slope_three).astype(jnp.bfloat16)
    g_three = jnp.einsum("td,tf->df", hidden, dz_three, preferred_element_type=jnp.float32)
    d_hidden = jnp.einsum("tf,df->td", dz_three, w_up[1], preferred_element_type=jnp.float32).astype(jnp.bfloat16)
    g_two = jnp.einsum("tf,td->fd", act_one, d_hidden, preferred_element_type=jnp.float32)
    dz_one = (jnp.einsum("td,fd->tf", d_hidden, w_down[0], preferred_element_type=jnp.float32) * slope_one).astype(jnp.bfloat16)
    g_one = jnp.einsum("td,tf->df", act_in, dz_one, preferred_element_type=jnp.float32)
    return g_one, g_two, g_three, g_four


def adam_direction(exp_avg, exp_sq, grad, clip_scale):
    bias_one = 1.0 - BETA_ONE ** STEP
    bias_two = 1.0 - BETA_TWO ** STEP
    avg_new = BETA_ONE * exp_avg + (1.0 - BETA_ONE) * clip_scale * grad
    sq_new = BETA_TWO * exp_sq + (1.0 - BETA_TWO) * (clip_scale * clip_scale) * (grad * grad)
    direction = (avg_new / bias_one) / (jnp.sqrt(sq_new / bias_two) + ADAM_EPS)
    return avg_new, sq_new, direction


class Unit:
    def __init__(self, kind, k, off, cols, order):
        self.kind, self.k, self.off, self.cols, self.order = kind, k, off, cols, order
        self.dims = "zy" if kind == "up" else "zyx"
        self.shape = (4,) * len(self.dims) + (48, cols)

    def half(self, phase, dest, h, me):
        if self.kind == "up" and phase == 2:
            return (dest, h), (6, self.cols)
        fixed = {d: me[d] for d in self.order[:phase]}
        fixed[self.order[phase]] = dest
        index, shape, split = [], [], False
        for d in self.dims:
            if d in fixed:
                index.append(fixed[d])
            elif not split:
                index.append(pl.ds(2 * h, 2))
                shape.append(2)
                split = True
            else:
                index.append(slice(None))
                shape.append(4)
        if split:
            return tuple(index), tuple(shape) + (48, self.cols)
        return tuple(index) + (pl.ds(24 * h, 24),), (24, self.cols)

    def half_shape(self, phase):
        return self.half(phase, 0, 0, dict(x=0, y=0, z=0))[1]


def make_units(up_cols, down_cols):
    u, d = up_cols // 2, down_cols // 3
    return [
        Unit("down", 1, 0, 2 * d, "xyz"),
        Unit("up", 1, 0, u, "zyx"),
        Unit("up", 1, u, u, "yzx"),
        Unit("down", 1, 2 * d, d, "yxz"),
        Unit("down", 0, 0, 2 * d, "xzy"),
        Unit("down", 0, 2 * d, d, "zxy"),
        Unit("up", 0, 0, u, "zyx"),
        Unit("up", 0, u, u, "yzx"),
    ]


def event_order(units):
    rate, hop, pair_rate, add_rate = 46600.0, 2.5, 550000.0, 1500000.0
    link, now, pair = {}, 0.0, 2.0
    ready, state, events = [], [], []
    size = [math.prod(u.shape) * 4 for u in units]
    for b in size:
        pair += b / pair_rate
        ready.append(pair)
        state.append(0)

    def send(d, sign, start, nbytes):
        key = (d, sign)
        link[key] = max(link.get(key, 0.0), start) + nbytes / rate
        return link[key] + hop

    last = [[0.0, 0.0] for _ in units]
    while any(s < 8 for s in state):
        i = min((j for j in range(len(units)) if state[j] < 8), key=lambda j: (ready[j], j))
        u, s = units[i], state[i]
        events.append((i, s))
        now = max(now, ready[i])
        if s == 0:
            now += 3 * size[i] / add_rate
        elif s < 7:
            phase = (s - 1) // 2
            now += 0.2 + 3 * size[i] / 4 ** (phase + 1) / add_rate
        if s < 7:
            phase = s // 2 if s % 2 == 0 else (s - 1) // 2
            if phase < 3:
                b = math.prod(u.half_shape(phase)) * 4
                d = u.order[phase]
                if s % 2 == 0:
                    arrive = [send(d, g, now, b) for g in (1, -1)]
                    last[i] = [send(d, g, now, b) for g in (1, -1)]
                    ready[i] = max(arrive)
                else:
                    arrive = [send(d, g, now, b) for g in (1, -1)]
                    ready[i] = max(arrive)
            else:
                ready[i] = now + 2.0
        state[i] += 1
    return events


def position():
    me = lax.axis_index("data")
    return dict(z=me // 32, y=(me // 8) % 4, x=(me // 2) % 4, c=me % 2)


def device_of(at):
    return (((at["z"] * 4 + at["y"]) * 4 + at["x"]) * 2 + at["c"],)


def moved(me, d, by):
    return device_of({**me, d: (me[d] + by) % 4})


def partner_of(me):
    return device_of({**me, "c": 1 - me["c"]})


def group_peers(me):
    first, second = [], []
    j, q = me["x"] * 2 + me["c"], me["z"] * 4 + me["y"]
    for t in range(1, 8):
        o = (j + t) % 8
        first.append((o, device_of({**me, "x": o // 2, "c": o % 2})))
    for t in range(1, 16):
        o = (q + t) % 16
        second.append((o, device_of({**me, "z": o // 4, "y": o % 4})))
    return first, second


def remote(src, dst, send_sem, recv_sem, device):
    return pltpu.make_async_remote_copy(src_ref=src, dst_ref=dst, send_sem=send_sem, recv_sem=recv_sem, device_id=device, device_id_type=MESH)


def add_into(dst, *srcs):
    lead = dst.shape[:-2]
    if not lead:
        dst[...] = functools.reduce(lambda a, b: a + b, [s[...] for s in srcs], dst[...])
        return

    def body(i, carry):
        index = []
        for n in reversed(lead):
            index.append(i % n)
            i = i // n
        index = tuple(reversed(index))
        dst[index] = functools.reduce(lambda a, b: a + b, [s[index] for s in srcs], dst[index])
        return carry

    lax.fori_loop(0, math.prod(lead), body, 0)


def reduce_update_kernel(units, events, *refs):
    n_units = len(units)
    take = iter(refs)
    g_ref = {("up", 0): next(take), ("down", 0): next(take), ("up", 1): next(take), ("down", 1): next(take)}
    master = dict(up=next(take), down=next(take))
    avg = dict(up=next(take), down=next(take))
    sq = dict(up=next(take), down=next(take))
    rate_ref, clip_ref = next(take), next(take)
    weight = dict(up=next(take), down=next(take))
    master_out = dict(up=next(take), down=next(take))
    avg_out = dict(up=next(take), down=next(take))
    sq_out = dict(up=next(take), down=next(take))
    norm_ref = next(take)
    acc = [next(take) for _ in units]
    recv = [[[next(take) for _ in range(6)] for _ in range(3)] for _ in units]
    xbuf = {i: next(take) for i, u in enumerate(units) if u.kind == "up"}
    fin = [next(take) for _ in units]
    slots = {}
    slot_of = {}
    for i, u in enumerate(units):
        if (u.kind, u.cols, u.off) not in slots:
            slots[u.kind, u.cols, u.off] = next(take)
        slot_of[i] = slots[u.kind, u.cols, u.off]
    grad = dict(up=next(take), down=next(take))
    small_src, small_one, small_two = next(take), next(take), next(take)
    load_sem, pair_send, pair_recv, ring_send, ring_recv, fin_send, fin_recv = [next(take) for _ in range(7)]
    one_send, one_recv, two_send, two_recv = [next(take) for _ in range(4)]

    me = position()
    core = me["c"]
    partner = partner_of(me)
    first, second = group_peers(me)

    barrier = pltpu.get_barrier_semaphore()
    for _, device in first + second:
        pl.semaphore_signal(barrier, inc=1, device_id=device, device_id_type=MESH)
    pl.semaphore_wait(barrier, len(first) + len(second))

    def columns(u, c):
        ref = g_ref[u.kind, u.k]
        width = ref.shape[-1] // 2
        start = pl.multiple_of(c * width + u.off, 128)
        return ref.at[(slice(None),) * (len(ref.shape) - 1) + (pl.ds(start, u.cols),)]

    pair_copy = [remote(columns(u, 1 - core), acc[i], pair_send.at[i], pair_recv.at[i], partner) for i, u in enumerate(units)]
    load_copy = [pltpu.make_async_copy(columns(u, core), slot_of[i], load_sem.at[i]) for i, u in enumerate(units)]
    later = {}
    for i, u in enumerate(units):
        earlier = [j for j in range(i) if slot_of[j] is slot_of[i]]
        if earlier:
            later[earlier[-1]] = i
        else:
            load_copy[i].start()
        pair_copy[i].start()

    sent = []

    def ring(i, phase, n):
        u = units[i]
        d = u.order[phase]
        base = xbuf[i] if u.kind == "up" and phase == 2 else acc[i]
        by = 1 if n % 2 == 0 else -1
        dest = (me[d] + (2 if n < 2 else by)) % 4
        h = (0, 1, 1, 0, 0, 1)[n]
        src = base.at[u.half(phase, dest, h, me)[0]]
        s = (i * 3 + phase) * 6 + n
        return remote(src, recv[i][phase][n], ring_send.at[s], ring_recv.at[s], moved(me, d, by)), src

    def start_phase(i, phase):
        u = units[i]
        if u.kind == "up" and phase == 2:
            block = acc[i][me["z"], me["y"]]
            for p in range(8):
                xbuf[i][p // 2, p % 2] = block[6 * p:6 * p + 6]
        for n in range(4):
            copy, _ = ring(i, phase, n)
            copy.start()
            sent.append(copy)

    for i, s in events:
        u = units[i]
        if s == 0:
            load_copy[i].wait()
            pair_copy[i].wait_recv()
            add_into(acc[i], slot_of[i])
            if i in later:
                load_copy[later[i]].start()
            start_phase(i, 0)
        elif s < 7 and s % 2 == 1:
            phase = (s - 1) // 2
            for n in (4, 5):
                copy, src = ring(i, phase, n)
                ring(i, phase, n - 4)[0].wait_recv()
                add_into(src, recv[i][phase][n - 4])
                copy.start()
                sent.append(copy)
        elif s < 7:
            phase = s // 2 - 1
            d = u.order[phase]
            base = xbuf[i] if u.kind == "up" and phase == 2 else acc[i]
            for n in (2, 3, 4, 5):
                ring(i, phase, n)[0].wait_recv()
            for h, (a, b) in enumerate(((4, 3), (2, 5))):
                add_into(base.at[u.half(phase, me[d], h, me)[0]], recv[i][phase][a], recv[i][phase][b])
            if phase < 2:
                start_phase(i, phase + 1)
            else:
                src = xbuf[i].at[me["x"], 1 - core] if u.kind == "up" else acc[i].at[me["z"], me["y"], me["x"], pl.ds(pl.multiple_of(24 * (1 - core), 8), 24)]
                copy = remote(src, fin[i], fin_send.at[i], fin_recv.at[i], partner)
                copy.start()
                sent.append(copy)
        else:
            src = xbuf[i].at[me["x"], core] if u.kind == "up" else acc[i].at[me["z"], me["y"], me["x"], pl.ds(pl.multiple_of(24 * core, 8), 24)]
            remote(src, fin[i], fin_send.at[i], fin_recv.at[i], partner).wait_recv()
            own, other = src[...], fin[i][...]
            half = grad[u.kind].shape[-1] // 2
            grad[u.kind][u.k, :, u.off:u.off + u.cols] = jnp.where(core == 0, own, other) * (1.0 / 128.0)
            grad[u.kind][u.k, :, half + u.off:half + u.off + u.cols] = jnp.where(core == 0, other, own) * (1.0 / 128.0)

    def total(values):
        row = lax.broadcasted_iota(jnp.int32, (8, 128), 0)
        tile = jnp.zeros((8, 128), F32)
        for r, value in enumerate(values):
            tile = jnp.where(row == r, value, tile)
        return tile

    def all_sum(at, tile):
        for stage, (peers, own, buf, send, recv_s) in enumerate((
            (first, me["x"] * 2 + core, small_one, one_send, one_recv),
            (second, me["z"] * 4 + me["y"], small_two, two_send, two_recv),
        )):
            small_src[at, stage] = tile
            buf[at, own] = tile
            for t, (o, device) in enumerate(peers):
                copy = remote(small_src.at[at, stage], buf.at[at, own], send.at[at, t], recv_s.at[at, own], device)
                copy.start()
                sent.append(copy)
            for o, device in peers:
                remote(small_src.at[at, stage], buf.at[at, o], send.at[at, 0], recv_s.at[at, o], device).wait_recv()
            tile = buf[at, 0]
            for o in range(1, len(peers) + 1):
                tile = tile + buf[at, o]
        return tile

    def squares(x):
        return jnp.sum(x * x)

    keys = (("up", 0), ("down", 0), ("up", 1), ("down", 1))
    local_sq = functools.reduce(lambda a, b: a + b, [squares(grad[kind][k]) for kind, k in keys])
    sums = all_sum(0, total([local_sq] + [squares(master[kind][k]) for kind, k in keys]))
    norm = jnp.sqrt(sums[0:1, :])
    norm_ref[...] = jnp.broadcast_to(norm, norm_ref.shape)
    clip_scale = jnp.minimum(1.0, clip_ref[0] / (norm + NORM_EPS))[:, 0:1]
    master_norm = jnp.sqrt(sums)
    local = []
    for kind, k in keys:
        avg_new, sq_new, direction = adam_direction(avg[kind][k], sq[kind][k], grad[kind][k], clip_scale)
        avg_out[kind][k] = avg_new
        sq_out[kind][k] = sq_new
        grad[kind][k] = direction
        local.append(squares(direction))
    dir_norm = jnp.sqrt(all_sum(1, total(local)))
    for r, (kind, k) in enumerate(keys):
        ratio = (master_norm[r + 1:r + 2, :] / dir_norm[r:r + 1, :])[:, 0:1]
        new = master[kind][k] - rate_ref[0] * ratio * grad[kind][k]
        master_out[kind][k] = new
        weight[kind][k] = new.astype(BF16)

    for copy in pair_copy + sent:
        copy.wait_send()


def reduce_update(grads, master, avg, sq, learn_rate, clip_norm):
    up_cols, down_cols = grads[0].shape[1], grads[1].shape[1]
    units = make_units(up_cols // 2, down_cols // 2)
    events = event_order(units)
    views = [g.reshape((4, 4, 48, up_cols)) if i % 2 == 0 else g.reshape((4, 4, 4, 48, down_cols)) for i, g in enumerate(grads)]
    scratch = [pltpu.VMEM(u.shape, F32) for u in units]
    scratch += [pltpu.VMEM(u.half_shape(p), F32) for u in units for p in range(3) for _ in range(6)]
    scratch += [pltpu.VMEM((4, 2, 6, u.cols), F32) for u in units if u.kind == "up"]
    scratch += [pltpu.VMEM((6 if u.kind == "up" else 24, u.cols), F32) for u in units]
    seen = set()
    for u in units:
        if (u.kind, u.cols, u.off) not in seen:
            seen.add((u.kind, u.cols, u.off))
            scratch.append(pltpu.VMEM(u.shape, F32))
    scratch += [pltpu.VMEM(master[0].shape, F32), pltpu.VMEM(master[1].shape, F32)]
    scratch += [pltpu.VMEM((2, 2, 8, 128), F32), pltpu.VMEM((2, 8, 8, 128), F32), pltpu.VMEM((2, 16, 8, 128), F32)]
    n = len(units)
    dma = pltpu.SemaphoreType.DMA
    scratch += [dma((n,)), dma((n,)), dma((n,)), dma((n * 18,)), dma((n * 18,)), dma((n,)), dma((n,))]
    scratch += [dma((2, 7)), dma((2, 8)), dma((2, 15)), dma((2, 16))]
    vmem, smem = pl.BlockSpec(memory_space=pltpu.VMEM), pl.BlockSpec(memory_space=pltpu.SMEM)
    state = [jax.ShapeDtypeStruct(a.shape, F32) for a in master]
    outs = pl.pallas_call(
        functools.partial(reduce_update_kernel, units, events),
        out_shape=[jax.ShapeDtypeStruct(a.shape, BF16) for a in master] + state * 3 + [jax.ShapeDtypeStruct((8, 128), F32)],
        in_specs=[pl.BlockSpec(memory_space=pl.ANY)] * 4 + [vmem] * 6 + [smem] * 2,
        out_specs=[vmem] * 9,
        scratch_shapes=scratch,
        compiler_params=pltpu.CompilerParams(collective_id=0, has_side_effects=True, vmem_limit_bytes=60 * 1024 * 1024),
        name="reduce_update",
    )(*views, *master, *avg, *sq, learn_rate.reshape(1), clip_norm.reshape(1))
    return outs


def solution(mesh):
    batch_rows = P("data", None)
    state_rows = P(None, "data", None)
    replicated = P()

    def device_step(act_in, grad_out, w_up, w_down, master_up, master_down, exp_avg_up, exp_avg_down, exp_sq_up, exp_sq_down, learn_rate, clip_norm):
        grads = local_grads(act_in, grad_out, w_up, w_down)
        outs = reduce_update(grads, (master_up, master_down), (exp_avg_up, exp_avg_down), (exp_sq_up, exp_sq_down), learn_rate, clip_norm)
        block_up, block_down, master_up_out, master_down_out, avg_up, avg_down, sq_up, sq_down, norm = outs
        new_w_up = lax.all_gather(block_up, "data", axis=1, tiled=True)
        new_w_down = lax.all_gather(block_down, "data", axis=1, tiled=True)
        return (new_w_up, new_w_down, master_up_out, master_down_out, avg_up, avg_down, sq_up, sq_down, norm[0, 0])

    return jax.shard_map(device_step, mesh=mesh, in_specs=(batch_rows, batch_rows, replicated, replicated, state_rows, state_rows, state_rows, state_rows, state_rows, state_rows, replicated, replicated), out_specs=(replicated, replicated, state_rows, state_rows, state_rows, state_rows, state_rows, state_rows, replicated), check_vma=False)
```

```python
import functools
import math

import jax
import jax.numpy as jnp
from jax import lax
from jax.experimental import pallas as pl
from jax.experimental.pallas import tpu as pltpu
from jax.sharding import PartitionSpec as P

STEP = 10
BETA_ONE = 0.9
BETA_TWO = 0.95
ADAM_EPS = 1e-8
NORM_EPS = 1e-6
INV_SQRT_TWO = 0.7071067811865476
INV_SQRT_TWO_PI = 0.3989422804014327

MESH = pl.DeviceIdType.MESH
RING = 4
ROWS = 48
HALF = 24
LANES = 128
F32 = jnp.float32
BF16 = jnp.bfloat16


def gelu_parts(pre_act):
    normal_cdf = 0.5 * (1.0 + lax.erf(pre_act * INV_SQRT_TWO))
    normal_pdf = jnp.exp(-0.5 * pre_act * pre_act) * INV_SQRT_TWO_PI
    return pre_act * normal_cdf, normal_cdf + pre_act * normal_pdf


def local_grads(act_in, grad_out, w_up, w_down):
    z_one = jnp.einsum("td,df->tf", act_in, w_up[0], preferred_element_type=jnp.float32)
    gelu_one, slope_one = gelu_parts(z_one)
    act_one = gelu_one.astype(jnp.bfloat16)
    hidden = jnp.einsum("tf,fd->td", act_one, w_down[0], preferred_element_type=jnp.float32).astype(jnp.bfloat16)
    z_three = jnp.einsum("td,df->tf", hidden, w_up[1], preferred_element_type=jnp.float32)
    gelu_three, slope_three = gelu_parts(z_three)
    act_three = gelu_three.astype(jnp.bfloat16)
    g_four = jnp.einsum("tf,td->fd", act_three, grad_out, preferred_element_type=jnp.float32)
    dz_three = (jnp.einsum("td,fd->tf", grad_out, w_down[1], preferred_element_type=jnp.float32) * slope_three).astype(jnp.bfloat16)
    g_three = jnp.einsum("td,tf->df", hidden, dz_three, preferred_element_type=jnp.float32)
    d_hidden = jnp.einsum("tf,df->td", dz_three, w_up[1], preferred_element_type=jnp.float32).astype(jnp.bfloat16)
    g_two = jnp.einsum("tf,td->fd", act_one, d_hidden, preferred_element_type=jnp.float32)
    dz_one = (jnp.einsum("td,fd->tf", d_hidden, w_down[0], preferred_element_type=jnp.float32) * slope_one).astype(jnp.bfloat16)
    g_one = jnp.einsum("td,tf->df", act_in, dz_one, preferred_element_type=jnp.float32)
    return g_one, g_two, g_three, g_four


def adam_direction(exp_avg, exp_sq, grad, clip_scale):
    bias_one = 1.0 - BETA_ONE ** STEP
    bias_two = 1.0 - BETA_TWO ** STEP
    avg_new = BETA_ONE * exp_avg + (1.0 - BETA_ONE) * clip_scale * grad
    sq_new = BETA_TWO * exp_sq + (1.0 - BETA_TWO) * (clip_scale * clip_scale) * (grad * grad)
    direction = (avg_new / bias_one) / (jnp.sqrt(sq_new / bias_two) + ADAM_EPS)
    return avg_new, sq_new, direction


class Unit:
    def __init__(self, kind, k, off, cols, order):
        self.kind, self.k, self.off, self.cols, self.order = kind, k, off, cols, order
        self.dims = "zy" if kind == "up" else "zyx"
        self.shape = (RING,) * len(self.dims) + (ROWS, cols)

    def half(self, phase, dest, h, me):
        if self.kind == "up" and phase == 2:
            return (dest, h), (6, self.cols)
        fixed = {d: me[d] for d in self.order[:phase]}
        fixed[self.order[phase]] = dest
        index, shape, split = [], [], False
        for d in self.dims:
            if d in fixed:
                index.append(fixed[d])
            elif not split:
                index.append(pl.ds(2 * h, 2))
                shape.append(2)
                split = True
            else:
                index.append(slice(None))
                shape.append(RING)
        if split:
            return tuple(index), tuple(shape) + (ROWS, self.cols)
        return tuple(index) + (pl.ds(HALF * h, HALF),), (HALF, self.cols)

    def half_shape(self, phase):
        return self.half(phase, 0, 0, dict(x=0, y=0, z=0))[1]


def make_units(up_cols, down_cols):
    u, d = up_cols // 2, down_cols // 3
    return [
        Unit("down", 1, 0, 2 * d, "xyz"),
        Unit("up", 1, 0, u, "zyx"),
        Unit("up", 1, u, u, "yzx"),
        Unit("down", 1, 2 * d, d, "yxz"),
        Unit("down", 0, 0, 2 * d, "xzy"),
        Unit("down", 0, 2 * d, d, "zxy"),
        Unit("up", 0, 0, u, "zyx"),
        Unit("up", 0, u, u, "yzx"),
    ]


def serve_order(ready, phases, tail):
    rate, hop, work = 46600.0, 2.5, 0.4
    link, now, events = {}, 0.0, []
    ready, state, late = list(ready), [0] * len(ready), [0.0] * len(ready)
    ends = [2 * len(p) + tail for p in phases]

    def send(phase):
        d, nbytes = phase
        for sign in "+-":
            link[d, sign] = max(link.get((d, sign), 0.0), now) + nbytes / rate
        return max(link[d, sign] for sign in "+-") + hop

    while any(s <= e for s, e in zip(state, ends)):
        i = min((j for j in range(len(ready)) if state[j] <= ends[j]), key=lambda j: (ready[j], j))
        phase, middle = divmod(state[i], 2)
        events.append((i, state[i]))
        now = max(now, ready[i]) + work
        if phase < len(phases[i]):
            ready[i] = send(phases[i][phase])
            if middle:
                ready[i] = max(ready[i], late[i])
            else:
                late[i] = send(phases[i][phase])
        else:
            ready[i] = now + hop
        state[i] += 1
    return events


def half_bytes(shape, dtype):
    return math.prod(shape) * jnp.dtype(dtype).itemsize


def position():
    me = lax.axis_index("data")
    return dict(z=me // 32, y=(me // 8) % RING, x=(me // 2) % RING, c=me % 2)


def device_of(at):
    return (((at["z"] * RING + at["y"]) * RING + at["x"]) * 2 + at["c"],)


def moved(me, d, by):
    return device_of({**me, d: (me[d] + by) % RING})


def partner_of(me):
    return device_of({**me, "c": 1 - me["c"]})


def group_peers(me):
    first, second = [], []
    j, q = me["x"] * 2 + me["c"], me["z"] * 4 + me["y"]
    for t in range(1, 8):
        o = (j + t) % 8
        first.append((o, device_of({**me, "x": o // 2, "c": o % 2})))
    for t in range(1, 16):
        o = (q + t) % 16
        second.append((o, device_of({**me, "z": o // 4, "y": o % RING})))
    return first, second


def remote(src, dst, send_sem, recv_sem, device):
    return pltpu.make_async_remote_copy(src_ref=src, dst_ref=dst, send_sem=send_sem, recv_sem=recv_sem, device_id=device, device_id_type=MESH)


def add_into(dst, *srcs):
    lead = dst.shape[:-2]
    if not lead:
        dst[...] = functools.reduce(lambda a, b: a + b, [s[...] for s in srcs], dst[...])
        return

    def body(i, carry):
        index = []
        for n in reversed(lead):
            index.append(i % n)
            i = i // n
        index = tuple(reversed(index))
        dst[index] = functools.reduce(lambda a, b: a + b, [s[index] for s in srcs], dst[index])
        return carry

    lax.fori_loop(0, math.prod(lead), body, 0)


def reduce_update_kernel(units, events, *refs):
    n_units = len(units)
    take = iter(refs)
    g_ref = {("up", 0): next(take), ("down", 0): next(take), ("up", 1): next(take), ("down", 1): next(take)}
    master = dict(up=next(take), down=next(take))
    avg = dict(up=next(take), down=next(take))
    sq = dict(up=next(take), down=next(take))
    rate_ref, clip_ref = next(take), next(take)
    weight = dict(up=next(take), down=next(take))
    master_out = dict(up=next(take), down=next(take))
    avg_out = dict(up=next(take), down=next(take))
    sq_out = dict(up=next(take), down=next(take))
    norm_ref = next(take)
    acc = [next(take) for _ in units]
    recv = [[[next(take) for _ in range(6)] for _ in range(3)] for _ in units]
    xbuf = {i: next(take) for i, u in enumerate(units) if u.kind == "up"}
    fin = [next(take) for _ in units]
    slots = {}
    slot_of = {}
    for i, u in enumerate(units):
        if (u.kind, u.cols, u.off) not in slots:
            slots[u.kind, u.cols, u.off] = next(take)
        slot_of[i] = slots[u.kind, u.cols, u.off]
    grad = dict(up=next(take), down=next(take))
    small_src, small_one, small_two = next(take), next(take), next(take)
    load_sem, pair_send, pair_recv, ring_send, ring_recv, fin_send, fin_recv = [next(take) for _ in range(7)]
    one_send, one_recv, two_send, two_recv = [next(take) for _ in range(4)]

    me = position()
    core = me["c"]
    partner = partner_of(me)
    first, second = group_peers(me)

    barrier = pltpu.get_barrier_semaphore()
    for _, device in first + second:
        pl.semaphore_signal(barrier, inc=1, device_id=device, device_id_type=MESH)
    pl.semaphore_wait(barrier, len(first) + len(second))

    def columns(u, c):
        ref = g_ref[u.kind, u.k]
        width = ref.shape[-1] // 2
        start = pl.multiple_of(c * width + u.off, LANES)
        return ref.at[(slice(None),) * (len(ref.shape) - 1) + (pl.ds(start, u.cols),)]

    pair_copy = [remote(columns(u, 1 - core), acc[i], pair_send.at[i], pair_recv.at[i], partner) for i, u in enumerate(units)]
    load_copy = [pltpu.make_async_copy(columns(u, core), slot_of[i], load_sem.at[i]) for i, u in enumerate(units)]
    later = {}
    for i, u in enumerate(units):
        earlier = [j for j in range(i) if slot_of[j] is slot_of[i]]
        if earlier:
            later[earlier[-1]] = i
        else:
            load_copy[i].start()
        pair_copy[i].start()

    sent = []

    def ring(i, phase, n):
        u = units[i]
        d = u.order[phase]
        base = xbuf[i] if u.kind == "up" and phase == 2 else acc[i]
        by = 1 if n % 2 == 0 else -1
        dest = (me[d] + (2 if n < 2 else by)) % RING
        h = (0, 1, 1, 0, 0, 1)[n]
        src = base.at[u.half(phase, dest, h, me)[0]]
        s = (i * 3 + phase) * 6 + n
        return remote(src, recv[i][phase][n], ring_send.at[s], ring_recv.at[s], moved(me, d, by)), src

    def start_phase(i, phase):
        u = units[i]
        if u.kind == "up" and phase == 2:
            block = acc[i][me["z"], me["y"]]
            for p in range(8):
                xbuf[i][p // 2, p % 2] = block[6 * p:6 * p + 6]
        for n in range(4):
            copy, _ = ring(i, phase, n)
            copy.start()
            sent.append(copy)

    for i, s in events:
        u = units[i]
        if s == 0:
            load_copy[i].wait()
            pair_copy[i].wait_recv()
            add_into(acc[i], slot_of[i])
            if i in later:
                load_copy[later[i]].start()
            start_phase(i, 0)
        elif s < 7 and s % 2 == 1:
            phase = (s - 1) // 2
            for n in (4, 5):
                copy, src = ring(i, phase, n)
                ring(i, phase, n - 4)[0].wait_recv()
                add_into(src, recv[i][phase][n - 4])
                copy.start()
                sent.append(copy)
        elif s < 7:
            phase = s // 2 - 1
            d = u.order[phase]
            base = xbuf[i] if u.kind == "up" and phase == 2 else acc[i]
            for n in (2, 3, 4, 5):
                ring(i, phase, n)[0].wait_recv()
            for h, (a, b) in enumerate(((4, 3), (2, 5))):
                add_into(base.at[u.half(phase, me[d], h, me)[0]], recv[i][phase][a], recv[i][phase][b])
            if phase < 2:
                start_phase(i, phase + 1)
            else:
                src = xbuf[i].at[me["x"], 1 - core] if u.kind == "up" else acc[i].at[me["z"], me["y"], me["x"], pl.ds(pl.multiple_of(HALF * (1 - core), 8), HALF)]
                copy = remote(src, fin[i], fin_send.at[i], fin_recv.at[i], partner)
                copy.start()
                sent.append(copy)
        else:
            src = xbuf[i].at[me["x"], core] if u.kind == "up" else acc[i].at[me["z"], me["y"], me["x"], pl.ds(pl.multiple_of(HALF * core, 8), HALF)]
            remote(src, fin[i], fin_send.at[i], fin_recv.at[i], partner).wait_recv()
            own, other = src[...], fin[i][...]
            half = grad[u.kind].shape[-1] // 2
            grad[u.kind][u.k, :, u.off:u.off + u.cols] = jnp.where(core == 0, own, other) * (1.0 / 128.0)
            grad[u.kind][u.k, :, half + u.off:half + u.off + u.cols] = jnp.where(core == 0, other, own) * (1.0 / 128.0)

    def total(values):
        row = lax.broadcasted_iota(jnp.int32, (8, LANES), 0)
        tile = jnp.zeros((8, LANES), F32)
        for r, value in enumerate(values):
            tile = jnp.where(row == r, value, tile)
        return tile

    def all_sum(at, tile):
        for stage, (peers, own, buf, send, recv_s) in enumerate((
            (first, me["x"] * 2 + core, small_one, one_send, one_recv),
            (second, me["z"] * 4 + me["y"], small_two, two_send, two_recv),
        )):
            small_src[at, stage] = tile
            buf[at, own] = tile
            for t, (o, device) in enumerate(peers):
                copy = remote(small_src.at[at, stage], buf.at[at, own], send.at[at, t], recv_s.at[at, own], device)
                copy.start()
                sent.append(copy)
            for o, device in peers:
                remote(small_src.at[at, stage], buf.at[at, o], send.at[at, 0], recv_s.at[at, o], device).wait_recv()
            tile = buf[at, 0]
            for o in range(1, len(peers) + 1):
                tile = tile + buf[at, o]
        return tile

    def squares(x):
        return jnp.sum(x * x)

    def rows(kind, k):
        return (slice(None), k) if kind == "up" else (k,)

    keys = (("up", 0), ("down", 0), ("up", 1), ("down", 1))
    local_sq = functools.reduce(lambda a, b: a + b, [squares(grad[kind][k]) for kind, k in keys])
    sums = all_sum(0, total([local_sq] + [squares(master[kind][rows(kind, k)]) for kind, k in keys]))
    norm = jnp.sqrt(sums[0:1, :])
    norm_ref[...] = jnp.broadcast_to(norm, norm_ref.shape)
    clip_scale = jnp.minimum(1.0, clip_ref[0] / (norm + NORM_EPS))[:, 0:1]
    master_norm = jnp.sqrt(sums)
    local = []
    for kind, k in keys:
        avg_new, sq_new, direction = adam_direction(avg[kind][rows(kind, k)], sq[kind][rows(kind, k)], grad[kind][k], clip_scale)
        avg_out[kind][rows(kind, k)] = avg_new
        sq_out[kind][rows(kind, k)] = sq_new
        grad[kind][k] = direction
        local.append(squares(direction))
    dir_norm = jnp.sqrt(all_sum(1, total(local)))
    for r, (kind, k) in enumerate(keys):
        ratio = (master_norm[r + 1:r + 2, :] / dir_norm[r:r + 1, :])[:, 0:1]
        new = master[kind][rows(kind, k)] - rate_ref[0] * ratio * grad[kind][k]
        master_out[kind][rows(kind, k)] = new
        weight[kind][k] = new.astype(BF16)

    for copy in pair_copy + sent:
        copy.wait_send()


def reduce_update(grads, master, avg, sq, learn_rate, clip_norm):
    up_cols, down_cols = grads[0].shape[1], grads[1].shape[1]
    units = make_units(up_cols // 2, down_cols // 2)
    arrive, ready = 2.0, []
    for u in units:
        arrive += half_bytes(u.shape, F32) / 550000.0
        ready.append(arrive)
    events = serve_order(ready, [[(u.order[p], half_bytes(u.half_shape(p), F32)) for p in range(3)] for u in units], 1)
    views = [g.reshape((RING, RING, ROWS, up_cols)) if i % 2 == 0 else g.reshape((RING, RING, RING, ROWS, down_cols)) for i, g in enumerate(grads)]
    scratch = [pltpu.VMEM(u.shape, F32) for u in units]
    scratch += [pltpu.VMEM(u.half_shape(p), F32) for u in units for p in range(3) for _ in range(6)]
    scratch += [pltpu.VMEM((4, 2, 6, u.cols), F32) for u in units if u.kind == "up"]
    scratch += [pltpu.VMEM((6 if u.kind == "up" else HALF, u.cols), F32) for u in units]
    seen = set()
    for u in units:
        if (u.kind, u.cols, u.off) not in seen:
            seen.add((u.kind, u.cols, u.off))
            scratch.append(pltpu.VMEM(u.shape, F32))
    master, avg, sq = [(up.transpose(1, 0, 2), down) for up, down in (master, avg, sq)]
    blocks = [(2, 6, up_cols), (2, HALF, down_cols)]
    scratch += [pltpu.VMEM(b, F32) for b in blocks]
    scratch += [pltpu.VMEM((2, 2, 8, LANES), F32), pltpu.VMEM((2, 8, 8, LANES), F32), pltpu.VMEM((2, 16, 8, LANES), F32)]
    n = len(units)
    dma = pltpu.SemaphoreType.DMA
    scratch += [dma((n,)), dma((n,)), dma((n,)), dma((n * 18,)), dma((n * 18,)), dma((n,)), dma((n,))]
    scratch += [dma((2, 7)), dma((2, 8)), dma((2, 15)), dma((2, 16))]
    vmem, smem = pl.BlockSpec(memory_space=pltpu.VMEM), pl.BlockSpec(memory_space=pltpu.SMEM)
    state = [jax.ShapeDtypeStruct(a.shape, F32) for a in master]
    outs = pl.pallas_call(
        functools.partial(reduce_update_kernel, units, events),
        out_shape=[jax.ShapeDtypeStruct(b, BF16) for b in blocks] + state * 3 + [jax.ShapeDtypeStruct((8, LANES), F32)],
        in_specs=[pl.BlockSpec(memory_space=pl.ANY)] * 4 + [vmem] * 6 + [smem] * 2,
        out_specs=[vmem] * 9,
        scratch_shapes=scratch,
        compiler_params=pltpu.CompilerParams(collective_id=0, has_side_effects=True, vmem_limit_bytes=60 * 1024 * 1024),
        name="reduce_update",
    )(*views, *master, *avg, *sq, learn_rate.reshape(1), clip_norm.reshape(1))
    return outs


class Gather:
    def __init__(self, kind, k, off, cols, order):
        self.kind, self.k, self.off, self.cols, self.order = kind, k, off, cols, order
        self.dims = "zy" if kind == "up" else "zyx"
        self.shape = (RING,) * len(self.dims) + (ROWS, cols)

    def chunk(self, phase, owner, me, h=None):
        gathered, d = self.order[:phase], self.order[phase]
        index, shape, split = [], [], h is None
        for e in self.dims:
            if e == d:
                index.append(owner)
            elif e not in gathered:
                index.append(me[e])
            elif split:
                index.append(slice(None))
                shape.append(RING)
            else:
                index.append(pl.ds(2 * h, 2))
                shape.append(2)
                split = True
        if split:
            return tuple(index), tuple(shape) + (ROWS, self.cols)
        return tuple(index) + (pl.ds(HALF * h, HALF),), (HALF, self.cols)


def make_gathers(up_cols, down_cols):
    u, d = up_cols // 2, down_cols // 3
    return [
        Gather("down", 1, 0, 2 * d, "zyx"),
        Gather("down", 0, 0, 2 * d, "yzx"),
        Gather("down", 1, 2 * d, d, "xzy"),
        Gather("down", 0, 2 * d, d, "xyz"),
        Gather("up", 1, 0, u, "yz"),
        Gather("up", 1, u, u, "zy"),
        Gather("up", 0, 0, u, "yz"),
        Gather("up", 0, u, u, "zy"),
    ]


def gather_kernel(units, events, up_ref, down_ref, out_up, out_down, *refs):
    take = iter(refs)
    block = [next(take) for _ in units]
    rows_up, rows_down, assembly = next(take), next(take), next(take)
    row_send, row_recv, core_send, core_recv, ring_send, ring_recv, own_sem, share_send, share_recv = [next(take) for _ in range(9)]
    me = position()
    core = me["c"]
    partner = partner_of(me)
    own = me["x"] * 2 + core
    first = group_peers(me)[0]
    around = [moved(me, d, by) for d in "zy" for by in (1, -1)]
    half_up, half_down = up_ref.shape[-1] // 2, down_ref.shape[-1] // 2

    barrier = pltpu.get_barrier_semaphore()
    for device in [device for _, device in first] + around:
        pl.semaphore_signal(barrier, inc=1, device_id=device, device_id_type=MESH)
    pl.semaphore_wait(barrier, len(first) + len(around))

    sent = []

    def send(copy):
        copy.start()
        sent.append(copy)

    other = pl.ds(pl.multiple_of((1 - core) * half_down, LANES), half_down)
    core_copy = remote(down_ref.at[:, :, other], rows_down, core_send, core_recv, partner)
    send(core_copy)
    for t, (o, device) in enumerate(first):
        width = pl.ds(pl.multiple_of((o % 2) * half_up, LANES), half_up)
        send(remote(up_ref.at[:, :, width], rows_up.at[own], row_send.at[t], row_recv.at[own], device))

    def part(i, phase, owner, h=None, of=core):
        u = units[i]
        out, half = (out_up, half_up) if u.kind == "up" else (out_down, half_down)
        at = u.chunk(phase, owner, me, h)[0]
        at = at + (slice(None),) * (len(u.dims) + 1 - len(at))
        return out.at[(u.k,) + at + (pl.ds(pl.multiple_of(of * half + u.off, LANES), u.cols),)]

    def ring(i, phase, n):
        d = units[i].order[phase]
        by = 1 if n % 2 == 0 else -1
        owner = me[d] if n < 4 else (me[d] - by) % RING
        ref = part(i, phase, owner, (0, 1, 1, 0, 0, 1)[n])
        s = (i * 3 + phase) * 6 + n
        return remote(ref, ref, ring_send.at[s], ring_recv.at[s], moved(me, d, by))

    def start_phase(i, phase):
        for n in range(4):
            send(ring(i, phase, n))

    shares = []

    def share(i, j, owner):
        phase = len(units[i].order) - 1
        mine, theirs = part(i, phase, owner), part(i, phase, owner, None, 1 - core)
        send(remote(mine, mine, share_send.at[i, j], share_recv.at[i, j], partner))
        shares.append(remote(theirs, theirs, share_send.at[i, j], share_recv.at[i, j], partner))

    rows_ready = [False]
    for i, s in events:
        u = units[i]
        last = len(u.order) - 1
        if s == 0:
            if u.kind == "down":
                if i == 0:
                    core_copy.wait_recv()
                low, high = down_ref[u.k, :, u.off:u.off + u.cols], down_ref[u.k, :, half_down + u.off:half_down + u.off + u.cols]
                mine = jnp.where(core == 0, low, high)
                theirs = rows_down[u.k, :, u.off:u.off + u.cols]
                block[i][...] = jnp.concatenate([jnp.where(core == 0, mine, theirs), jnp.where(core == 0, theirs, mine)], axis=0)
            else:
                if not rows_ready[0]:
                    rows_ready[0] = True
                    rows_up[own] = jnp.where(core == 0, up_ref[:, :, :half_up], up_ref[:, :, half_up:])
                    for o, device in first:
                        remote(rows_up.at[o], rows_up.at[o], row_send.at[0], row_recv.at[o], device).wait_recv()
                for p in range(8):
                    assembly[6 * p:6 * p + 6, :] = rows_up[p, u.k, :, u.off:u.off + u.cols].astype(F32)
                block[i][...] = assembly[...].astype(BF16)
            own_copy = pltpu.make_async_copy(block[i], part(i, 0, me[u.order[0]]), own_sem.at[i])
            own_copy.start()
            own_copy.wait()
            start_phase(i, 0)
        elif s % 2 == 1:
            phase = (s - 1) // 2
            if phase == last:
                share(i, 0, me[u.order[last]])
            for n in (4, 5):
                d = u.order[phase]
                incoming = part(i, phase, (me[d] + (-1 if n == 4 else 1)) % RING, n - 4)
                remote(incoming, incoming, ring_send.at[0], ring_recv.at[(i * 3 + phase) * 6 + n - 4], moved(me, d, 1)).wait_recv()
                send(ring(i, phase, n))
        else:
            phase = s // 2 - 1
            d = u.order[phase]
            for n in (2, 3, 4, 5):
                step = {2: -1, 3: 1, 4: -2, 5: 2}[n]
                h = {2: 1, 3: 0, 4: 0, 5: 1}[n]
                incoming = part(i, phase, (me[d] + step) % RING, h)
                remote(incoming, incoming, ring_send.at[0], ring_recv.at[(i * 3 + phase) * 6 + n], moved(me, d, 1)).wait_recv()
                if phase == last and n == 3:
                    share(i, 1, (me[d] - 1) % RING)
                    share(i, 2, (me[d] + 1) % RING)
            if phase < last:
                start_phase(i, phase + 1)
            else:
                share(i, 3, (me[d] + 2) % RING)

    for copy in shares:
        copy.wait_recv()
    for copy in sent:
        copy.wait_send()


def gather_weights(block_up, block_down):
    up_cols, down_cols = block_up.shape[2], block_down.shape[2]
    units = make_gathers(up_cols // 2, down_cols // 2)
    here = dict(x=0, y=0, z=0)
    events = serve_order([2.0 if u.kind == "down" else 6.0 for u in units], [[(d, half_bytes(u.chunk(p, 0, here, 0)[1], BF16)) for p, d in enumerate(u.order)] for u in units], 0)
    n = len(units)
    dma = pltpu.SemaphoreType.DMA
    scratch = [pltpu.VMEM((ROWS, u.cols), BF16) for u in units]
    scratch += [pltpu.VMEM((8, 2, 6, up_cols // 2), BF16), pltpu.VMEM((2, HALF, down_cols // 2), BF16), pltpu.VMEM((ROWS, up_cols // 4), F32)]
    scratch += [dma((7,)), dma((8,)), dma, dma, dma((n * 18,)), dma((n * 18,)), dma((n,)), dma((n, 4)), dma((n, 4))]
    vmem = pl.BlockSpec(memory_space=pltpu.VMEM)
    out_up, out_down = pl.pallas_call(
        functools.partial(gather_kernel, units, events),
        out_shape=[jax.ShapeDtypeStruct((2, RING, RING, ROWS, up_cols), BF16), jax.ShapeDtypeStruct((2, RING, RING, RING, ROWS, down_cols), BF16)],
        in_specs=[vmem] * 2,
        out_specs=[pl.BlockSpec(memory_space=pl.ANY)] * 2,
        scratch_shapes=scratch,
        compiler_params=pltpu.CompilerParams(collective_id=1, has_side_effects=True, vmem_limit_bytes=HALF * 1024 * 1024),
        name="gather_weights",
    )(block_up, block_down)
    return out_up, out_down


def finish_kernel(*refs):
    n = (len(refs) - 1) // 2
    copies = []
    for i in range(n):
        src, dst = refs[i], refs[n + i]
        for j in range(src.shape[0] * 2 if len(src.shape) > 3 else 1):
            at = (j // 2, pl.ds(j % 2 * 2, 2)) if len(src.shape) > 3 else slice(None)
            copies.append(pltpu.make_async_copy(src.at[at], dst.at[at], refs[-1].at[i, j]))
    for copy in copies:
        copy.start()
    for copy in copies:
        copy.wait()


def finish(arrays):
    any_space = pl.BlockSpec(memory_space=pl.ANY)
    return pl.pallas_call(
        finish_kernel,
        out_shape=[jax.ShapeDtypeStruct(a.shape, a.dtype) for a in arrays],
        in_specs=[any_space] * len(arrays),
        out_specs=[any_space] * len(arrays),
        scratch_shapes=[pltpu.SemaphoreType.DMA((len(arrays), 4))],
        compiler_params=pltpu.CompilerParams(vmem_limit_bytes=1024 * 1024),
        name="finish",
    )(*arrays)


def solution(mesh):
    batch_rows = P("data", None)
    state_rows = P(None, "data", None)
    replicated = P()

    def device_step(act_in, grad_out, w_up, w_down, master_up, master_down, exp_avg_up, exp_avg_down, exp_sq_up, exp_sq_down, learn_rate, clip_norm):
        grads = local_grads(act_in, grad_out, w_up, w_down)
        outs = reduce_update(grads, (master_up, master_down), (exp_avg_up, exp_avg_down), (exp_sq_up, exp_sq_down), learn_rate, clip_norm)
        new_w_up, new_w_down, *state, norm = finish((*gather_weights(*outs[:2]), *outs[2:]))
        state = [a.transpose(1, 0, 2) if i % 2 == 0 else a for i, a in enumerate(state)]
        return (new_w_up.reshape(w_up.shape), new_w_down.reshape(w_down.shape), *state, norm[0, 0])

    return jax.shard_map(device_step, mesh=mesh, in_specs=(batch_rows, batch_rows, replicated, replicated, state_rows, state_rows, state_rows, state_rows, state_rows, state_rows, replicated, replicated), out_specs=(replicated, replicated, state_rows, state_rows, state_rows, state_rows, state_rows, state_rows, replicated), check_vma=False)
```

```python
import functools
import math

import jax
import jax.numpy as jnp
from jax import lax
from jax.experimental import pallas as pl
from jax.experimental.pallas import tpu as pltpu
from jax.sharding import PartitionSpec as P

STEP = 10
BETA_ONE = 0.9
BETA_TWO = 0.95
ADAM_EPS = 1e-8
NORM_EPS = 1e-6
INV_SQRT_TWO = 0.7071067811865476
INV_SQRT_TWO_PI = 0.3989422804014327

MESH = pl.DeviceIdType.MESH
RING = 4
ROWS = 48
HALF = 24
LANES = 128
PAIR = 2
PHASES = 3
SENDS = 6
F32 = jnp.float32
BF16 = jnp.bfloat16


def gelu_parts(pre_act):
    normal_cdf = 0.5 * (1.0 + lax.erf(pre_act * INV_SQRT_TWO))
    normal_pdf = jnp.exp(-0.5 * pre_act * pre_act) * INV_SQRT_TWO_PI
    return pre_act * normal_cdf, normal_cdf + pre_act * normal_pdf


def forward(act_in, w_up, w_down):
    z_one = jnp.einsum("td,df->tf", act_in, w_up[0], preferred_element_type=jnp.float32)
    gelu_one, slope_one = gelu_parts(z_one)
    act_one = gelu_one.astype(jnp.bfloat16)
    hidden = jnp.einsum("tf,fd->td", act_one, w_down[0], preferred_element_type=jnp.float32).astype(jnp.bfloat16)
    z_three = jnp.einsum("td,df->tf", hidden, w_up[1], preferred_element_type=jnp.float32)
    gelu_three, slope_three = gelu_parts(z_three)
    return act_one, slope_one, hidden, gelu_three.astype(jnp.bfloat16), slope_three


def adam_direction(exp_avg, exp_sq, grad, clip_scale):
    bias_one = 1.0 - BETA_ONE ** STEP
    bias_two = 1.0 - BETA_TWO ** STEP
    avg_new = BETA_ONE * exp_avg + (1.0 - BETA_ONE) * clip_scale * grad
    sq_new = BETA_TWO * exp_sq + (1.0 - BETA_TWO) * (clip_scale * clip_scale) * (grad * grad)
    direction = (avg_new / bias_one) / (jnp.sqrt(sq_new / bias_two) + ADAM_EPS)
    return avg_new, sq_new, direction


class Unit:
    def __init__(self, kind, k, off, cols, order):
        self.kind, self.k, self.off, self.cols, self.order = kind, k, off, cols, order
        self.dims = "zy" if kind == "up" else "zyx"
        self.shape = (RING,) * len(self.dims) + (ROWS, cols)

    def half(self, phase, dest, h, me):
        if self.kind == "up" and phase == 2:
            return (dest, h), (6, self.cols)
        fixed = {d: me[d] for d in self.order[:phase]}
        fixed[self.order[phase]] = dest
        index, shape, split = [], [], False
        for d in self.dims:
            if d in fixed:
                index.append(fixed[d])
            elif not split:
                index.append(pl.ds(PAIR * h, 2))
                shape.append(2)
                split = True
            else:
                index.append(slice(None))
                shape.append(RING)
        if split:
            return tuple(index), tuple(shape) + (ROWS, self.cols)
        return tuple(index) + (pl.ds(HALF * h, HALF),), (HALF, self.cols)

    def half_shape(self, phase):
        return self.half(phase, 0, 0, dict(x=0, y=0, z=0))[1]


def make_units(up_cols, down_cols):
    u, d = up_cols // PAIR, down_cols // 3
    return [
        Unit("down", 1, 0, PAIR * d, "xyz"),
        Unit("down", 1, PAIR * d, d, "xzy"),
        Unit("up", 1, 0, u, "zyx"),
        Unit("up", 1, u, u, "yzx"),
        Unit("up", 0, 0, u, "zyx"),
        Unit("up", 0, u, u, "yzx"),
        Unit("down", 0, 0, d, "xyz"),
        Unit("down", 0, d, d, "yzx"),
        Unit("down", 0, PAIR * d, d, "zxy"),
    ]


def serve_order(slots, ready, phases, tail, moved_per_us):
    rate, hop = 43000.0, 3.0
    link, now, plan = {}, 0.0, []
    ready, state, late = list(ready), [0] * len(ready), [0.0] * len(ready)
    ends = [PAIR * len(p) + tail for p in phases]

    def send(phase):
        d, nbytes = phase
        for sign in "+-":
            link[d, sign] = max(link.get((d, sign), 0.0), now) + nbytes / rate
        return max(link[d, sign] for sign in "+-") + hop

    for duration, starts in list(slots) + [(None, ())]:
        served = []
        while True:
            open_units = [j for j in range(len(ready)) if state[j] <= ends[j] and ready[j] is not None]
            if not open_units:
                break
            i = min(open_units, key=lambda j: (ready[j], j))
            if duration is not None and ready[i] > now:
                break
            phase, middle = divmod(state[i], 2)
            served.append((i, state[i]))
            now = max(now, ready[i])
            if state[i]:
                now += 0.3 + 8 * phases[i][(state[i] - 1) // PAIR if state[i] <= PAIR * len(phases[i]) else -1][1] / moved_per_us
            if phase < len(phases[i]):
                ready[i] = send(phases[i][phase])
                if middle:
                    ready[i] = max(ready[i], late[i])
                else:
                    late[i] = send(phases[i][phase])
            else:
                ready[i] = now + hop
            state[i] += 1
        plan.append(served)
        if duration is not None:
            now += duration
            for i in starts:
                ready[i] = now
    return plan


def half_bytes(shape, dtype):
    return math.prod(shape) * jnp.dtype(dtype).itemsize


def position():
    me = lax.axis_index("data")
    return dict(z=me // 32, y=(me // 8) % RING, x=(me // PAIR) % RING, c=me % PAIR)


def device_of(at):
    return (((at["z"] * RING + at["y"]) * RING + at["x"]) * 2 + at["c"],)


def moved(me, d, by):
    return device_of({**me, d: (me[d] + by) % RING})


def partner_of(me):
    return device_of({**me, "c": 1 - me["c"]})


def group_peers(me):
    first, second = [], []
    j, q = me["x"] * 2 + me["c"], me["z"] * 4 + me["y"]
    for t in range(1, 8):
        o = (j + t) % 8
        first.append((o, device_of({**me, "x": o // PAIR, "c": o % PAIR})))
    for t in range(1, 16):
        o = (q + t) % 16
        second.append((o, device_of({**me, "z": o // 4, "y": o % RING})))
    return first, second


def remote(src, dst, send_sem, recv_sem, device):
    return pltpu.make_async_remote_copy(src_ref=src, dst_ref=dst, send_sem=send_sem, recv_sem=recv_sem, device_id=device, device_id_type=MESH)


def add_into(dst, *srcs):
    lead = dst.shape[:-2]
    if not lead:
        dst[...] = functools.reduce(lambda a, b: a + b, [s[...] for s in srcs], dst[...])
        return

    def body(i, carry):
        index = []
        for n in reversed(lead):
            index.append(i % n)
            i = i // n
        index = tuple(reversed(index))
        dst[index] = functools.reduce(lambda a, b: a + b, [s[index] for s in srcs], dst[index])
        return carry

    lax.fori_loop(0, math.prod(lead), body, 0)


def dot(a, b, contract):
    return lax.dot_general(a, b, ((contract[:1], contract[1:]), ((), ())), preferred_element_type=F32)


def grad_update_kernel(units, plan, *refs):
    take = iter(refs)
    act_in, grad_out, hidden, act_one, act_three, slope_one, slope_three, w_up, w_down = [next(take) for _ in range(9)]
    master = dict(up=next(take), down=next(take))
    avg = dict(up=next(take), down=next(take))
    sq = dict(up=next(take), down=next(take))
    rate_ref, clip_ref = next(take), next(take)
    weight = dict(up=next(take), down=next(take))
    master_out = dict(up=next(take), down=next(take))
    avg_out = dict(up=next(take), down=next(take))
    sq_out = dict(up=next(take), down=next(take))
    norm_ref = next(take)
    acc_up = next(take)
    acc = [acc_up.at[1 - u.k, int(u.off > 0)] if u.kind == "up" else next(take) for u in units]
    recv = [[[next(take) for _ in range(SENDS)] for _ in range(PHASES)] for _ in units]
    xbuf = {i: next(take) for i, u in enumerate(units) if u.kind == "up"}
    fin = [next(take) for _ in units]
    grad = dict(up=next(take), down=next(take))
    small_src, small_one, small_two = next(take), next(take), next(take)
    stage_down, stage_up, inner, right, outer, w_tile, s_tile, a_tile, w_wide = [next(take) for _ in range(9)]
    down_send, down_recv, up_send, up_recv, ring_send, ring_recv, fin_send, fin_recv = [next(take) for _ in range(8)]
    one_send, one_recv, two_send, two_recv = [next(take) for _ in range(4)]
    w_sem, s_sem, a_sem, load_sem = [next(take) for _ in range(4)]

    me = position()
    core = me["c"]
    partner = partner_of(me)
    first, second = group_peers(me)
    n_tiles, piece_cols, wide = 12, w_tile.shape[1], a_tile.shape[2]
    down_half = grad["down"].shape[-1] // PAIR

    load_right = pltpu.make_async_copy(grad_out, right, load_sem.at[0])
    load_outer = pltpu.make_async_copy(hidden, outer, load_sem.at[1])
    load_next = pltpu.make_async_copy(act_in, outer, load_sem.at[1])

    def load_wide(n):
        rows = pl.ds(pl.multiple_of(n * piece_cols, piece_cols), piece_cols)
        return pltpu.make_async_copy(w_up.at[1, rows], w_wide, load_sem.at[2])

    def load_a(source, t):
        return pltpu.make_async_copy(source.at[:, pl.ds(pl.multiple_of(t % 8 * wide, LANES), wide)], a_tile.at[t % PAIR], a_sem.at[t % PAIR])

    def tile_columns(t):
        half = jnp.where(t < n_tiles // PAIR, 1 - core, core)
        return pl.ds(pl.multiple_of((half * (n_tiles // PAIR) + t % (n_tiles // PAIR)) * piece_cols, piece_cols), piece_cols)

    def load_tile(at, wait):
        stage, slot, cols = at // n_tiles, at % PAIR, tile_columns(at % n_tiles)
        w_copy = pltpu.make_async_copy(w_down.at[1 - stage, cols], w_tile.at[slot], w_sem.at[slot])
        if wait:
            w_copy.wait()
            pltpu.make_async_copy(slope_one.at[:, cols], s_tile.at[slot], s_sem.at[slot]).wait()
            return
        w_copy.start()
        for n, source in enumerate((slope_three, slope_one)):
            pl.when(stage == n)(pltpu.make_async_copy(source.at[:, cols], s_tile.at[slot], s_sem.at[slot]).start)

    load_right.start()
    load_a(act_three, 0).start()
    load_outer.start()
    load_tile(0, False)
    load_wide(0).start()

    barrier = pltpu.get_barrier_semaphore()
    for _, device in first + second:
        pl.semaphore_signal(barrier, inc=1, device_id=device, device_id_type=MESH)
    pl.semaphore_wait(barrier, len(first) + len(second))

    sent = []

    def ring(i, phase, n):
        u = units[i]
        d = u.order[phase]
        base = xbuf[i] if u.kind == "up" and phase == 2 else acc[i]
        by = 1 if n % PAIR == 0 else -1
        dest = (me[d] + (2 if n < 2 else by)) % RING
        h = (0, 1, 1, 0, 0, 1)[n]
        src = base.at[u.half(phase, dest, h, me)[0]]
        s = (i * PHASES + phase) * SENDS + n
        return remote(src, recv[i][phase][n], ring_send.at[s], ring_recv.at[s], moved(me, d, by))

    def last_piece(i, c):
        u = units[i]
        if u.kind == "up":
            return xbuf[i].at[me["x"], c]
        return acc[i].at[me["z"], me["y"], me["x"], pl.ds(pl.multiple_of(HALF * c, 8), HALF)]

    def swap(i):
        return remote(last_piece(i, 1 - core), fin[i], fin_send.at[i], fin_recv.at[i], partner)

    def send(make):
        make().start()
        sent.append(make)

    def start_phase(i, phase):
        u = units[i]
        if u.kind == "up" and phase == 2:
            block = acc[i][me["z"], me["y"]]
            for p in range(8):
                xbuf[i][p // PAIR, p % PAIR] = block[6 * p:6 * p + 6]
        for n in range(4):
            send(functools.partial(ring, i, phase, n))

    def serve(i, s):
        u = units[i]
        if s == 0:
            start_phase(i, 0)
        elif s < 7 and s % PAIR == 1:
            phase = (s - 1) // PAIR
            d = u.order[phase]
            base = xbuf[i] if u.kind == "up" and phase == 2 else acc[i]
            for n in (4, 5):
                ring(i, phase, n - 4).wait_recv()
                dest = (me[d] + (1 if n == 4 else -1)) % RING
                add_into(base.at[u.half(phase, dest, n - 4, me)[0]], recv[i][phase][n - 4])
                send(functools.partial(ring, i, phase, n))
        elif s < 7:
            phase = s // PAIR - 1
            d = u.order[phase]
            base = xbuf[i] if u.kind == "up" and phase == 2 else acc[i]
            for n in (PAIR, 3, 4, 5):
                ring(i, phase, n).wait_recv()
            for h, (a, b) in enumerate(((4, 3), (PAIR, 5))):
                add_into(base.at[u.half(phase, me[d], h, me)[0]], recv[i][phase][a], recv[i][phase][b])
            if phase < 2:
                start_phase(i, phase + 1)
            else:
                send(functools.partial(swap, i))
        else:
            swap(i).wait_recv()
            own, other = last_piece(i, core)[...], fin[i][...]
            half = grad[u.kind].shape[-1] // PAIR
            grad[u.kind][u.k, :, u.off:u.off + u.cols] = jnp.where(core == 0, own, other) * (1.0 / 128.0)
            grad[u.kind][u.k, :, half + u.off:half + u.off + u.cols] = jnp.where(core == 0, other, own) * (1.0 / 128.0)

    def serve_at(t, steps):
        if steps:
            @pl.when(t[0] == t[1])
            def _():
                for i, s in steps:
                    serve(i, s)

    def down_piece(i, z):
        u = units[i]
        return remote(stage_down.at[z, :, :, :, u.off:u.off + u.cols], acc[i].at[z], down_send.at[i, z], down_recv.at[i, z], partner)

    def down_grad(source, following, group, steps):
        def tile(t, carry):
            for k, served in enumerate(steps):
                serve_at((t, k), served)
            load_a(source, t).wait()
            pl.when(t < 15)(lambda: load_a(source, t + 1).start())
            if following is not None:
                pl.when(t == 15)(lambda: load_a(following, 0).start())
            columns = jnp.where(t < 8, 1 - core, core)
            value = dot(a_tile[t % PAIR], right[:, pl.ds(pl.multiple_of(columns * down_half, LANES), down_half)], (0, 0))
            value = value.reshape(PAIR, RING, ROWS, down_half)
            z, y = t % 8 // PAIR, pl.ds(t % PAIR * 2, 2)

            @pl.when(t < 8)
            def _():
                stage_down[z, y] = value
                pl.when(t % PAIR == 1)(lambda: [down_piece(i, z).start() for i in group] and None)

            @pl.when(t >= 8)
            def _():
                pl.when(t % PAIR == 0)(lambda: [down_piece(i, z).wait_recv() for i in group] and None)
                for i in group:
                    acc[i][z, y] += value[..., units[i].off:units[i].off + units[i].cols]
            return carry

        lax.fori_loop(0, 16, tile, 0)

    def up_piece(n):
        cols = pl.ds(pl.multiple_of(n % 3 * piece_cols, piece_cols), piece_cols)
        return remote(stage_up.at[:, :, :, cols], acc_up.at[n // 6, n // 3 % PAIR, :, :, :, cols], up_send.at[n], up_recv.at[n], partner)

    def up_tile(at, carry):
        for k, steps in enumerate(plan["up"]):
            serve_at((at, k), steps)

        @pl.when(at == n_tiles)
        def _():
            load_next.start()
            for n in range(PHASES):
                load_wide(n).wait()
                right[:, n * piece_cols:(n + 1) * piece_cols] = dot(inner[...], w_wide[...], (1, 1)).astype(BF16)
                if n < 2:
                    load_wide(n + 1).start()
            load_next.wait()

        load_tile(at, True)
        pl.when(at < PAIR * n_tiles - 1)(lambda: load_tile(at + 1, False))
        stage, t = at // n_tiles, at % n_tiles
        cols = tile_columns(t)
        inner[:, cols] = (dot(right[...], w_tile[at % PAIR], (1, 1)) * s_tile[at % PAIR]).astype(BF16)
        n = stage * 6 + t % 6
        place = pl.ds(pl.multiple_of(t % 3 * piece_cols, piece_cols), piece_cols)
        pl.when((t < 6) & (n > 2))(lambda: up_piece(n - 3).wait_send())
        pl.when(t >= 6)(lambda: up_piece(n).wait_recv())
        rows = outer.shape[1] // PAIR
        for r in range(2):
            value = dot(outer[:, r * rows:(r + 1) * rows], inner[:, cols], (0, 0)).reshape(PAIR, RING, ROWS, piece_cols)

            @pl.when(t < 6)
            def _():
                stage_up[PAIR * r:PAIR * r + 2, :, :, place] = value

            @pl.when(t >= 6)
            def _():
                acc_up[stage, t // 3 % PAIR, PAIR * r:PAIR * r + 2, :, :, place] += value
        pl.when(t < 6)(lambda: up_piece(n).start())
        return carry

    load_right.wait()
    down_grad(act_three, act_one, (0, 1), ())
    load_outer.wait()
    lax.fori_loop(0, PAIR * n_tiles, up_tile, 0)
    for i in (0, 1):
        for z in range(RING):
            down_piece(i, z).wait_send()
    down_grad(act_one, None, (6, 7, 8), plan["down"])
    for i, s in plan["end"]:
        serve(i, s)

    def total(values):
        row = lax.broadcasted_iota(jnp.int32, (8, LANES), 0)
        tile = jnp.zeros((8, LANES), F32)
        for r, value in enumerate(values):
            tile = jnp.where(row == r, value, tile)
        return tile

    def all_sum(at, tile):
        for stage, (peers, own, buf, send_s, recv_s) in enumerate((
            (first, me["x"] * 2 + core, small_one, one_send, one_recv),
            (second, me["z"] * RING + me["y"], small_two, two_send, two_recv),
        )):
            small_src[at, stage] = tile
            buf[at, own] = tile
            for t, (o, device) in enumerate(peers):
                send(functools.partial(remote, small_src.at[at, stage], buf.at[at, own], send_s.at[at, t], recv_s.at[at, own], device))
            for o, device in peers:
                remote(small_src.at[at, stage], buf.at[at, o], send_s.at[at, 0], recv_s.at[at, o], device).wait_recv()
            tile = buf[at, 0]
            for o in range(1, len(peers) + 1):
                tile = tile + buf[at, o]
        return tile

    def squares(x):
        return jnp.sum(x * x)

    def rows(kind, k):
        return (slice(None), k) if kind == "up" else (k,)

    keys = (("up", 0), ("down", 0), ("up", 1), ("down", 1))
    local_sq = functools.reduce(lambda a, b: a + b, [squares(grad[kind][k]) for kind, k in keys])
    sums = all_sum(0, total([local_sq] + [squares(master[kind][rows(kind, k)]) for kind, k in keys]))
    norm = jnp.sqrt(sums[0:1, :])
    norm_ref[...] = jnp.broadcast_to(norm, norm_ref.shape)
    clip_scale = jnp.minimum(1.0, clip_ref[0] / (norm + NORM_EPS))[:, 0:1]
    master_norm = jnp.sqrt(sums)
    local = []
    for kind, k in keys:
        avg_new, sq_new, direction = adam_direction(avg[kind][rows(kind, k)], sq[kind][rows(kind, k)], grad[kind][k], clip_scale)
        avg_out[kind][rows(kind, k)] = avg_new
        sq_out[kind][rows(kind, k)] = sq_new
        grad[kind][k] = direction
        local.append(squares(direction))
    dir_norm = jnp.sqrt(all_sum(1, total(local)))
    for r, (kind, k) in enumerate(keys):
        ratio = (master_norm[r + 1:r + 2, :] / dir_norm[r:r + 1, :])[:, 0:1]
        new = master[kind][rows(kind, k)] - rate_ref[0] * ratio * grad[kind][k]
        master_out[kind][rows(kind, k)] = new
        weight[kind][k] = new.astype(BF16)

    for i in (6, 7, 8):
        for z in range(RING):
            down_piece(i, z).wait_send()
    for n in range(9, 12):
        up_piece(n).wait_send()
    for make in sent:
        make().wait_send()


def grad_update(tensors, master, avg, sq, learn_rate, clip_norm):
    tokens, down_cols = tensors[0].shape
    up_cols = tensors[3].shape[1]
    units = make_units(up_cols // PAIR, down_cols // PAIR)
    phases = [[(u.order[p], half_bytes(u.half_shape(p), F32)) for p in range(PHASES)] for u in units]
    slots = [(12.0, (0, 1))]
    slots += [(1.3 + (t == 11) * 7, {8: (2,), 11: (3,), 20: (4,), 23: (5,)}.get(t, ())) for t in range(24)]
    slots += [(0.75, (6, 7, 8) if t == 15 else ()) for t in range(16)]
    steps = serve_order(slots, [None] * len(units), phases, 1, 1500000.0)
    plan = dict(up=steps[1:25], down=steps[25:41], end=steps[41])
    master, avg, sq = [(up.transpose(1, 0, 2), down) for up, down in (master, avg, sq)]
    blocks = [(PAIR, 6, up_cols), (PAIR, HALF, down_cols)]
    piece = up_cols // 12
    scratch = [pltpu.VMEM((PAIR, 2, RING, RING, ROWS, up_cols // RING), F32)]
    scratch += [pltpu.VMEM(u.shape, F32) for u in units if u.kind == "down"]
    scratch += [pltpu.VMEM(u.half_shape(p), F32) for u in units for p in range(PHASES) for _ in range(SENDS)]
    scratch += [pltpu.VMEM((RING, 2, 6, u.cols), F32) for u in units if u.kind == "up"]
    scratch += [pltpu.VMEM((6 if u.kind == "up" else HALF, u.cols), F32) for u in units]
    scratch += [pltpu.VMEM(b, F32) for b in blocks]
    scratch += [pltpu.VMEM((PAIR, 2, 8, LANES), F32), pltpu.VMEM((PAIR, 8, 8, LANES), F32), pltpu.VMEM((PAIR, 16, 8, LANES), F32)]
    scratch += [pltpu.VMEM((RING, RING, RING, ROWS, down_cols // PAIR), F32), pltpu.VMEM((RING, RING, ROWS, 3 * piece), F32)]
    scratch += [pltpu.VMEM((tokens, up_cols), BF16), pltpu.VMEM((tokens, down_cols), BF16), pltpu.VMEM((tokens, down_cols), BF16)]
    scratch += [pltpu.VMEM((PAIR, piece, down_cols), BF16), pltpu.VMEM((PAIR, tokens, piece), F32)]
    scratch += [pltpu.VMEM((PAIR, tokens, up_cols // 8), BF16), pltpu.VMEM((piece, up_cols), BF16)]
    n = len(units)
    dma = pltpu.SemaphoreType.DMA
    scratch += [dma((n, RING)), dma((n, RING)), dma((12,)), dma((12,)), dma((n * PHASES * SENDS,)), dma((n * PHASES * SENDS,)), dma((n,)), dma((n,))]
    scratch += [dma((PAIR, 7)), dma((PAIR, 8)), dma((PAIR, 15)), dma((PAIR, 16)), dma((2,)), dma((2,)), dma((2,)), dma((3,))]
    vmem, smem, any_space = [pl.BlockSpec(memory_space=s) for s in (pltpu.VMEM, pltpu.SMEM, pl.ANY)]
    state = [jax.ShapeDtypeStruct(a.shape, F32) for a in master]
    return pl.pallas_call(
        functools.partial(grad_update_kernel, units, plan),
        out_shape=[jax.ShapeDtypeStruct(b, BF16) for b in blocks] + state * 3 + [jax.ShapeDtypeStruct((8, LANES), F32)],
        in_specs=[any_space] * len(tensors) + [vmem] * 6 + [smem] * 2,
        out_specs=[vmem] * 9,
        scratch_shapes=scratch,
        compiler_params=pltpu.CompilerParams(collective_id=0, has_side_effects=True, vmem_limit_bytes=67043328),
        name="grad_update",
    )(*tensors, *master, *avg, *sq, learn_rate.reshape(1), clip_norm.reshape(1))


class Gather:
    def __init__(self, kind, k, off, cols, order):
        self.kind, self.k, self.off, self.cols, self.order = kind, k, off, cols, order
        self.dims = "zy" if kind == "up" else "zyx"
        self.shape = (RING,) * len(self.dims) + (ROWS, cols)

    def chunk(self, phase, owner, me, h=None):
        gathered, d = self.order[:phase], self.order[phase]
        index, shape, split = [], [], h is None
        for e in self.dims:
            if e == d:
                index.append(owner)
            elif e not in gathered:
                index.append(me[e])
            elif split:
                index.append(slice(None))
                shape.append(RING)
            else:
                index.append(pl.ds(PAIR * h, 2))
                shape.append(2)
                split = True
        if split:
            return tuple(index), tuple(shape) + (ROWS, self.cols)
        return tuple(index) + (pl.ds(HALF * h, HALF),), (HALF, self.cols)


def make_gathers(up_cols, down_cols):
    u, d = up_cols // PAIR, down_cols // 3
    return [
        Gather("down", 1, 0, PAIR * d, "zyx"),
        Gather("down", 0, 0, PAIR * d, "yzx"),
        Gather("down", 1, PAIR * d, d, "xzy"),
        Gather("down", 0, PAIR * d, d, "xyz"),
        Gather("up", 1, 0, u, "yz"),
        Gather("up", 1, u, u, "zy"),
        Gather("up", 0, 0, u, "yz"),
        Gather("up", 0, u, u, "zy"),
    ]


def gather_kernel(units, events, up_ref, down_ref, out_up, out_down, *refs):
    take = iter(refs)
    block = [next(take) for _ in units]
    rows_up, rows_down, assembly = next(take), next(take), next(take)
    row_send, row_recv, core_send, core_recv, ring_send, ring_recv, own_sem, share_send, share_recv = [next(take) for _ in range(9)]
    me = position()
    core = me["c"]
    partner = partner_of(me)
    own = me["x"] * 2 + core
    first = group_peers(me)[0]
    around = [moved(me, d, by) for d in "zy" for by in (1, -1)]
    half_up, half_down = up_ref.shape[-1] // PAIR, down_ref.shape[-1] // PAIR

    barrier = pltpu.get_barrier_semaphore()
    for device in [device for _, device in first] + around:
        pl.semaphore_signal(barrier, inc=1, device_id=device, device_id_type=MESH)
    pl.semaphore_wait(barrier, len(first) + len(around))

    sent = []

    def send(copy):
        copy.start()
        sent.append(copy)

    other = pl.ds(pl.multiple_of((1 - core) * half_down, LANES), half_down)
    core_copy = remote(down_ref.at[:, :, other], rows_down, core_send, core_recv, partner)
    send(core_copy)
    for t, (o, device) in enumerate(first):
        width = pl.ds(pl.multiple_of((o % PAIR) * half_up, LANES), half_up)
        send(remote(up_ref.at[:, :, width], rows_up.at[own], row_send.at[t], row_recv.at[own], device))

    def part(i, phase, owner, h=None, of=core):
        u = units[i]
        out, half = (out_up, half_up) if u.kind == "up" else (out_down, half_down)
        at = u.chunk(phase, owner, me, h)[0]
        at = at + (slice(None),) * (len(u.dims) + 1 - len(at))
        return out.at[(u.k,) + at + (pl.ds(pl.multiple_of(of * half + u.off, LANES), u.cols),)]

    def ring(i, phase, n):
        d = units[i].order[phase]
        by = 1 if n % PAIR == 0 else -1
        owner = me[d] if n < 4 else (me[d] - by) % RING
        ref = part(i, phase, owner, (0, 1, 1, 0, 0, 1)[n])
        s = (i * PHASES + phase) * SENDS + n
        return remote(ref, ref, ring_send.at[s], ring_recv.at[s], moved(me, d, by))

    def start_phase(i, phase):
        for n in range(4):
            send(ring(i, phase, n))

    shares = []

    def share(i, j, owner):
        phase = len(units[i].order) - 1
        mine, theirs = part(i, phase, owner), part(i, phase, owner, None, 1 - core)
        send(remote(mine, mine, share_send.at[i, j], share_recv.at[i, j], partner))
        shares.append(remote(theirs, theirs, share_send.at[i, j], share_recv.at[i, j], partner))

    rows_ready = [False]
    for i, s in events:
        u = units[i]
        last = len(u.order) - 1
        if s == 0:
            if u.kind == "down":
                if i == 0:
                    core_copy.wait_recv()
                low, high = down_ref[u.k, :, u.off:u.off + u.cols], down_ref[u.k, :, half_down + u.off:half_down + u.off + u.cols]
                mine = jnp.where(core == 0, low, high)
                theirs = rows_down[u.k, :, u.off:u.off + u.cols]
                block[i][...] = jnp.concatenate([jnp.where(core == 0, mine, theirs), jnp.where(core == 0, theirs, mine)], axis=0)
            else:
                if not rows_ready[0]:
                    rows_ready[0] = True
                    rows_up[own] = jnp.where(core == 0, up_ref[:, :, :half_up], up_ref[:, :, half_up:])
                    for o, device in first:
                        remote(rows_up.at[o], rows_up.at[o], row_send.at[0], row_recv.at[o], device).wait_recv()
                for p in range(8):
                    assembly[6 * p:6 * p + 6, :] = rows_up[p, u.k, :, u.off:u.off + u.cols].astype(F32)
                block[i][...] = assembly[...].astype(BF16)
            own_copy = pltpu.make_async_copy(block[i], part(i, 0, me[u.order[0]]), own_sem.at[i])
            own_copy.start()
            own_copy.wait()
            start_phase(i, 0)
        elif s % PAIR == 1:
            phase = (s - 1) // PAIR
            if phase == last:
                share(i, 0, me[u.order[last]])
            for n in (4, 5):
                d = u.order[phase]
                incoming = part(i, phase, (me[d] + (-1 if n == 4 else 1)) % RING, n - 4)
                remote(incoming, incoming, ring_send.at[0], ring_recv.at[(i * PHASES + phase) * SENDS + n - 4], moved(me, d, 1)).wait_recv()
                send(ring(i, phase, n))
        else:
            phase = s // PAIR - 1
            d = u.order[phase]
            for n in (PAIR, 3, 4, 5):
                step = {2: -1, 3: 1, 4: -2, 5: 2}[n]
                h = {2: 1, 3: 0, 4: 0, 5: 1}[n]
                incoming = part(i, phase, (me[d] + step) % RING, h)
                remote(incoming, incoming, ring_send.at[0], ring_recv.at[(i * PHASES + phase) * SENDS + n], moved(me, d, 1)).wait_recv()
                if phase == last and n == 3:
                    share(i, 1, (me[d] - 1) % RING)
                    share(i, 2, (me[d] + 1) % RING)
            if phase < last:
                start_phase(i, phase + 1)
            else:
                share(i, 3, (me[d] + 2) % RING)

    for copy in shares:
        copy.wait_recv()
    for copy in sent:
        copy.wait_send()


def gather_weights(block_up, block_down):
    up_cols, down_cols = block_up.shape[2], block_down.shape[2]
    units = make_gathers(up_cols // PAIR, down_cols // PAIR)
    here = dict(x=0, y=0, z=0)
    phases = [[(d, half_bytes(u.chunk(p, 0, here, 0)[1], BF16)) for p, d in enumerate(u.order)] for u in units]
    events = serve_order((), [2.0 if u.kind == "down" else 6.0 for u in units], phases, 0, math.inf)[0]
    n = len(units)
    dma = pltpu.SemaphoreType.DMA
    scratch = [pltpu.VMEM((ROWS, u.cols), BF16) for u in units]
    scratch += [pltpu.VMEM((8, 2, 6, up_cols // PAIR), BF16), pltpu.VMEM((PAIR, HALF, down_cols // PAIR), BF16), pltpu.VMEM((ROWS, up_cols // 4), F32)]
    scratch += [dma((7,)), dma((8,)), dma, dma, dma((n * PHASES * SENDS,)), dma((n * PHASES * SENDS,)), dma((n,)), dma((n, 4)), dma((n, 4))]
    vmem = pl.BlockSpec(memory_space=pltpu.VMEM)
    out_up, out_down = pl.pallas_call(
        functools.partial(gather_kernel, units, events),
        out_shape=[jax.ShapeDtypeStruct((PAIR, RING, RING, ROWS, up_cols), BF16), jax.ShapeDtypeStruct((PAIR, RING, RING, RING, ROWS, down_cols), BF16)],
        in_specs=[vmem] * 2,
        out_specs=[pl.BlockSpec(memory_space=pl.ANY)] * 2,
        scratch_shapes=scratch,
        compiler_params=pltpu.CompilerParams(collective_id=1, has_side_effects=True, vmem_limit_bytes=HALF * 1024 * 1024),
        name="gather_weights",
    )(block_up, block_down)
    return out_up, out_down


def finish_kernel(*refs):
    n = (len(refs) - 1) // PAIR
    copies = []
    for i in range(n):
        src, dst = refs[i], refs[n + i]
        for j in range(src.shape[0] * 2 if len(src.shape) > 3 else 1):
            at = (j // PAIR, pl.ds(j % PAIR * 2, 2)) if len(src.shape) > 3 else slice(None)
            copies.append(pltpu.make_async_copy(src.at[at], dst.at[at], refs[-1].at[i, j]))
    for copy in copies:
        copy.start()
    for copy in copies:
        copy.wait()


def finish(arrays):
    any_space = pl.BlockSpec(memory_space=pl.ANY)
    return pl.pallas_call(
        finish_kernel,
        out_shape=[jax.ShapeDtypeStruct(a.shape, a.dtype) for a in arrays],
        in_specs=[any_space] * len(arrays),
        out_specs=[any_space] * len(arrays),
        scratch_shapes=[pltpu.SemaphoreType.DMA((len(arrays), 4))],
        compiler_params=pltpu.CompilerParams(vmem_limit_bytes=1024 * 1024),
        name="finish",
    )(*arrays)


def solution(mesh):
    batch_rows = P("data", None)
    state_rows = P(None, "data", None)
    replicated = P()

    def device_step(act_in, grad_out, w_up, w_down, master_up, master_down, exp_avg_up, exp_avg_down, exp_sq_up, exp_sq_down, learn_rate, clip_norm):
        act_one, slope_one, hidden, act_three, slope_three = forward(act_in, w_up, w_down)
        tensors = (act_in, grad_out, hidden, act_one, act_three, slope_one, slope_three, w_up, w_down)
        outs = grad_update(tensors, (master_up, master_down), (exp_avg_up, exp_avg_down), (exp_sq_up, exp_sq_down), learn_rate, clip_norm)
        new_w_up, new_w_down, *state, norm = finish((*gather_weights(*outs[:2]), *outs[2:]))
        state = [a.transpose(1, 0, 2) if i % PAIR == 0 else a for i, a in enumerate(state)]
        return (new_w_up.reshape(w_up.shape), new_w_down.reshape(w_down.shape), *state, norm[0, 0])

    return jax.shard_map(device_step, mesh=mesh, in_specs=(batch_rows, batch_rows, replicated, replicated, state_rows, state_rows, state_rows, state_rows, state_rows, state_rows, replicated, replicated), out_specs=(replicated, replicated, state_rows, state_rows, state_rows, state_rows, state_rows, state_rows, replicated), check_vma=False)
```

```python
import functools
import math

import jax
import jax.numpy as jnp
from jax import lax
from jax.experimental import pallas as pl
from jax.experimental.pallas import tpu as pltpu
from jax.sharding import PartitionSpec as P

STEP = 10
BETA_ONE = 0.9
BETA_TWO = 0.95
ADAM_EPS = 1e-8
NORM_EPS = 1e-6
INV_SQRT_TWO = 0.7071067811865476
INV_SQRT_TWO_PI = 0.3989422804014327

MESH = pl.DeviceIdType.MESH
RING = 4
ROWS = 48
HALF = 24
LANES = 128
PAIR = 2
PHASES = 3
FULL_VMEM = 67043328
WEIGHT_LIMIT = 4194304
AHEAD = 4
SENDS = 6
F32 = jnp.float32
BF16 = jnp.bfloat16


def gelu_parts(pre_act):
    normal_cdf = 0.5 * (1.0 + lax.erf(pre_act * INV_SQRT_TWO))
    normal_pdf = jnp.exp(-0.5 * pre_act * pre_act) * INV_SQRT_TWO_PI
    return pre_act * normal_cdf, normal_cdf + pre_act * normal_pdf


def forward(act_in, w_up, w_down):
    z_one = jnp.einsum("td,df->tf", act_in, w_up[0], preferred_element_type=jnp.float32)
    gelu_one, slope_one = gelu_parts(z_one)
    act_one = gelu_one.astype(jnp.bfloat16)
    hidden = jnp.einsum("tf,fd->td", act_one, w_down[0], preferred_element_type=jnp.float32).astype(jnp.bfloat16)
    z_three = jnp.einsum("td,df->tf", hidden, w_up[1], preferred_element_type=jnp.float32)
    gelu_three, slope_three = gelu_parts(z_three)
    return act_one, slope_one, hidden, gelu_three.astype(jnp.bfloat16), slope_three


def adam_direction(exp_avg, exp_sq, grad, clip_scale):
    bias_one = 1.0 - BETA_ONE ** STEP
    bias_two = 1.0 - BETA_TWO ** STEP
    avg_new = BETA_ONE * exp_avg + (1.0 - BETA_ONE) * clip_scale * grad
    sq_new = BETA_TWO * exp_sq + (1.0 - BETA_TWO) * (clip_scale * clip_scale) * (grad * grad)
    direction = (avg_new / bias_one) / (jnp.sqrt(sq_new / bias_two) + ADAM_EPS)
    return avg_new, sq_new, direction


class Unit:
    def __init__(self, kind, k, off, cols, order):
        self.kind, self.k, self.off, self.cols, self.order = kind, k, off, cols, order
        self.dims = "zy" if kind == "up" else "zyx"
        self.shape = (RING,) * len(self.dims) + (ROWS, cols)

    def half(self, phase, dest, h, me):
        if self.kind == "up" and phase == 2:
            return (dest, h), (6, self.cols)
        fixed = {d: me[d] for d in self.order[:phase]}
        fixed[self.order[phase]] = dest
        index, shape, split = [], [], False
        for d in self.dims:
            if d in fixed:
                index.append(fixed[d])
            elif not split:
                index.append(pl.ds(PAIR * h, 2))
                shape.append(2)
                split = True
            else:
                index.append(slice(None))
                shape.append(RING)
        if split:
            return tuple(index), tuple(shape) + (ROWS, self.cols)
        return tuple(index) + (pl.ds(HALF * h, HALF),), (HALF, self.cols)

    def half_shape(self, phase):
        return self.half(phase, 0, 0, dict(x=0, y=0, z=0))[1]


def column_groups(make, specs, up_cols, down_cols):
    groups = []
    for spec in specs:
        k, first, count = map(int, spec[1:4])
        kind, part = ("up", up_cols // PAIR) if spec[0] == "u" else ("down", down_cols // 3)
        groups.append(make(kind, k, first * part, count * part, spec[4:]))
    return groups


REDUCE = ("d102xyz", "d121zyx", "u101zyx", "u111yzx")
REDUCE_LATE = ("u001zyx", "u011yzx", "d001zyx", "d011xyz", "d021xyz")
GATHER = ("d102zyx", "d002yzx", "d121xzy", "d021xyz")
GATHER_LATE = ("u101yz", "u111zy", "u001yz", "u011zy")


def serve_order(slots, ready, phases, tail, moved_per_us):
    rate, hop = 44000.0, 3.0
    link, now, plan = {}, 0.0, []
    ready, state, late = list(ready), [0] * len(ready), [0.0] * len(ready)
    ends = [PAIR * len(p) + tail for p in phases]

    def send(phase):
        d, nbytes = phase
        for sign in "+-":
            link[d, sign] = max(link.get((d, sign), 0.0), now) + nbytes / rate
        return max(link[d, sign] for sign in "+-") + hop

    for duration, starts in list(slots) + [(None, ())]:
        served = []
        while True:
            open_units = [j for j in range(len(ready)) if state[j] <= ends[j] and ready[j] is not None]
            if not open_units:
                break
            i = min(open_units, key=lambda j: (ready[j], j))
            if duration is not None and ready[i] > now:
                break
            phase, middle = divmod(state[i], 2)
            served.append((i, state[i]))
            now = max(now, ready[i])
            if state[i]:
                now += 0.05 + 8 * phases[i][(state[i] - 1) // PAIR if state[i] <= PAIR * len(phases[i]) else -1][1] / moved_per_us
            if phase < len(phases[i]):
                ready[i] = send(phases[i][phase])
                if middle:
                    ready[i] = max(ready[i], late[i])
                else:
                    late[i] = send(phases[i][phase])
            else:
                ready[i] = now + hop
            state[i] += 1
        plan.append(served)
        if duration is not None:
            now += duration
            for i in starts:
                ready[i] = now
    return plan


def half_bytes(shape, dtype):
    return math.prod(shape) * jnp.dtype(dtype).itemsize


def position():
    me = lax.axis_index("data")
    return dict(z=me // 32, y=(me // 8) % RING, x=(me // PAIR) % RING, c=me % PAIR)


def device_of(at):
    return (((at["z"] * RING + at["y"]) * RING + at["x"]) * 2 + at["c"],)


def moved(me, d, by):
    return device_of({**me, d: (me[d] + by) % RING})


def partner_of(me):
    return device_of({**me, "c": 1 - me["c"]})


def group_peers(me):
    first, second = [], []
    j, q = me["x"] * 2 + me["c"], me["z"] * 4 + me["y"]
    for t in range(1, 8):
        o = (j + t) % 8
        first.append((o, device_of({**me, "x": o // PAIR, "c": o % PAIR})))
    for t in range(1, 16):
        o = (q + t) % 16
        second.append((o, device_of({**me, "z": o // 4, "y": o % RING})))
    return first, second


def remote(src, dst, send_sem, recv_sem, device):
    return pltpu.make_async_remote_copy(src_ref=src, dst_ref=dst, send_sem=send_sem, recv_sem=recv_sem, device_id=device, device_id_type=MESH)


def add_into(dst, *srcs):
    lead = dst.shape[:-2]
    if not lead:
        dst[...] = functools.reduce(lambda a, b: a + b, [s[...] for s in srcs], dst[...])
        return

    def body(i, carry):
        index = []
        for n in reversed(lead):
            index.append(i % n)
            i = i // n
        index = tuple(reversed(index))
        dst[index] = functools.reduce(lambda a, b: a + b, [s[index] for s in srcs], dst[index])
        return carry

    lax.fori_loop(0, math.prod(lead), body, 0)


def dot(a, b, contract):
    return lax.dot_general(a, b, ((contract[:1], contract[1:]), ((), ())), preferred_element_type=F32)


def grad_update_kernel(units, plan, *refs):
    take = iter(refs)
    act_in, grad_out, hidden, act_one, act_three, slope_one, slope_three, w_up, w_down = [next(take) for _ in range(9)]
    master = dict(up=next(take), down=next(take))
    avg = dict(up=next(take), down=next(take))
    sq = dict(up=next(take), down=next(take))
    rate_ref, clip_ref = next(take), next(take)
    weight = dict(up=next(take), down=next(take))
    master_out = dict(up=next(take), down=next(take))
    avg_out = dict(up=next(take), down=next(take))
    sq_out = dict(up=next(take), down=next(take))
    norm_ref = next(take)
    acc_up = next(take)
    acc = [acc_up.at[1 - u.k, int(u.off > 0)] if u.kind == "up" else next(take) for u in units]
    recv = [[[next(take) for _ in range(SENDS)] for _ in range(PHASES)] for _ in units]
    xbuf = {i: next(take) for i, u in enumerate(units) if u.kind == "up"}
    fin = [next(take) for _ in units]
    grad = dict(up=next(take), down=next(take))
    small_src, small_one, small_two = next(take), next(take), next(take)
    stage_down, stage_up, inner, right, outer, w_tile, s_tile, a_tile, w_wide = [next(take) for _ in range(9)]
    down_send, down_recv, up_send, up_recv, ring_send, ring_recv, fin_send, fin_recv = [next(take) for _ in range(8)]
    one_send, one_recv, two_send, two_recv = [next(take) for _ in range(4)]
    w_sem, s_sem, a_sem, load_sem = [next(take) for _ in range(4)]

    me = position()
    core = me["c"]
    partner = partner_of(me)
    first, second = group_peers(me)
    n_tiles, piece_cols, wide = 12, w_tile.shape[1], a_tile.shape[2]
    down_half = grad["down"].shape[-1] // PAIR

    load_right = pltpu.make_async_copy(grad_out, right, load_sem.at[0])
    load_outer = pltpu.make_async_copy(hidden, outer, load_sem.at[1])
    load_next = pltpu.make_async_copy(act_in, outer, load_sem.at[1])

    def load_wide(n):
        rows = pl.ds(pl.multiple_of(n * piece_cols, piece_cols), piece_cols)
        return pltpu.make_async_copy(w_up.at[1, rows], w_wide, load_sem.at[2])

    def load_a(source, t):
        return pltpu.make_async_copy(source.at[:, pl.ds(pl.multiple_of(t % 8 * wide, LANES), wide)], a_tile.at[t % AHEAD], a_sem.at[t % AHEAD])

    def tile_columns(t):
        half = jnp.where(t < n_tiles // PAIR, 1 - core, core)
        return pl.ds(pl.multiple_of((half * (n_tiles // PAIR) + t % (n_tiles // PAIR)) * piece_cols, piece_cols), piece_cols)

    def load_tile(at, wait):
        stage, slot, cols = at // n_tiles, at % PAIR, tile_columns(at % n_tiles)
        w_copy = pltpu.make_async_copy(w_down.at[1 - stage, cols], w_tile.at[slot], w_sem.at[slot])
        if wait:
            w_copy.wait()
            pltpu.make_async_copy(slope_one.at[:, cols], s_tile.at[slot], s_sem.at[slot]).wait()
            return
        w_copy.start()
        for n, source in enumerate((slope_three, slope_one)):
            pl.when(stage == n)(pltpu.make_async_copy(source.at[:, cols], s_tile.at[slot], s_sem.at[slot]).start)

    load_right.start()
    for t in range(AHEAD - 1):
        load_a(act_three, t).start()
    load_outer.start()
    load_tile(0, False)
    load_wide(0).start()

    barrier = pltpu.get_barrier_semaphore()
    for _, device in first + second:
        pl.semaphore_signal(barrier, inc=1, device_id=device, device_id_type=MESH)
    pl.semaphore_wait(barrier, len(first) + len(second))

    sent = []

    def ring(i, phase, n):
        u = units[i]
        d = u.order[phase]
        base = xbuf[i] if u.kind == "up" and phase == 2 else acc[i]
        by = 1 if n % PAIR == 0 else -1
        dest = (me[d] + (2 if n < 2 else by)) % RING
        h = (0, 1, 1, 0, 0, 1)[n]
        src = base.at[u.half(phase, dest, h, me)[0]]
        s = (i * PHASES + phase) * SENDS + n
        return remote(src, recv[i][phase][n], ring_send.at[s], ring_recv.at[s], moved(me, d, by))

    def last_piece(i, c):
        u = units[i]
        if u.kind == "up":
            return xbuf[i].at[me["x"], c]
        return acc[i].at[me["z"], me["y"], me["x"], pl.ds(pl.multiple_of(HALF * c, 8), HALF)]

    def swap(i):
        return remote(last_piece(i, 1 - core), fin[i], fin_send.at[i], fin_recv.at[i], partner)

    def send(make):
        make().start()
        sent.append(make)

    def start_phase(i, phase):
        u = units[i]
        if u.kind == "up" and phase == 2:
            block = acc[i][me["z"], me["y"]]
            for p in range(8):
                xbuf[i][p // PAIR, p % PAIR] = block[6 * p:6 * p + 6]
        for n in range(4):
            send(functools.partial(ring, i, phase, n))

    def serve(i, s):
        u = units[i]
        if s == 0:
            start_phase(i, 0)
        elif s < 7 and s % PAIR == 1:
            phase = (s - 1) // PAIR
            d = u.order[phase]
            base = xbuf[i] if u.kind == "up" and phase == 2 else acc[i]
            for n in (4, 5):
                ring(i, phase, n - 4).wait_recv()
                dest = (me[d] + (1 if n == 4 else -1)) % RING
                add_into(base.at[u.half(phase, dest, n - 4, me)[0]], recv[i][phase][n - 4])
                send(functools.partial(ring, i, phase, n))
        elif s < 7:
            phase = s // PAIR - 1
            d = u.order[phase]
            base = xbuf[i] if u.kind == "up" and phase == 2 else acc[i]
            for n in (PAIR, 3, 4, 5):
                ring(i, phase, n).wait_recv()
            for h, (a, b) in enumerate(((4, 3), (PAIR, 5))):
                add_into(base.at[u.half(phase, me[d], h, me)[0]], recv[i][phase][a], recv[i][phase][b])
            if phase < 2:
                start_phase(i, phase + 1)
            else:
                send(functools.partial(swap, i))
        else:
            swap(i).wait_recv()
            own, other = last_piece(i, core)[...], fin[i][...]
            half = grad[u.kind].shape[-1] // PAIR
            grad[u.kind][u.k, :, u.off:u.off + u.cols] = jnp.where(core == 0, own, other) * (1.0 / 128.0)
            grad[u.kind][u.k, :, half + u.off:half + u.off + u.cols] = jnp.where(core == 0, other, own) * (1.0 / 128.0)

    def serve_at(t, steps):
        if steps:
            @pl.when(t[0] == t[1])
            def _():
                for i, s in steps:
                    serve(i, s)

    def down_piece(i, z):
        u = units[i]
        return remote(stage_down.at[z, :, :, :, u.off:u.off + u.cols], acc[i].at[z], down_send.at[i, z], down_recv.at[i, z], partner)

    def down_grad(source, following, group, mine, steps):
        columns = core if mine else 1 - core

        def tile(t, carry):
            for k, served in enumerate(steps):
                serve_at((t, k), served)
            z, y = t // PAIR, pl.ds(t % PAIR * 2, 2)
            if mine:
                pl.when(t % PAIR == 0)(lambda: [down_piece(i, z).wait_recv() for i in group] and None)
            load_a(source, t).wait()
            later = t + AHEAD - 1
            pl.when(later < 8)(lambda: load_a(source, later).start())
            if following is not None:
                pl.when(later >= 8)(lambda: load_a(following, later).start())
            value = dot(a_tile[t % AHEAD], right[:, pl.ds(pl.multiple_of(columns * down_half, LANES), down_half)], (0, 0))
            value = value.reshape(PAIR, RING, ROWS, down_half)
            if mine:
                for i in group:
                    acc[i][z, y] += value[..., units[i].off:units[i].off + units[i].cols]
            else:
                stage_down[z, y] = value
                pl.when(t % PAIR == 1)(lambda: [down_piece(i, z).start() for i in group] and None)
            return carry

        lax.fori_loop(0, 8, tile, 0)

    def up_piece(n):
        cols = pl.ds(pl.multiple_of(n % 3 * piece_cols, piece_cols), piece_cols)
        return remote(stage_up.at[:, :, :, cols], acc_up.at[n // 6, n // 3 % PAIR, :, :, :, cols], up_send.at[n], up_recv.at[n], partner)

    def up_grad(stage, mine, steps):
        start = stage * n_tiles + mine * 6

        def tile(t, carry):
            for k, served in enumerate(steps):
                serve_at((t, k), served)
            at = start + t
            n = stage * 6 + t
            if mine:
                up_piece(n).wait_recv()
            else:
                pl.when(n > 2)(lambda: up_piece(n - 3).wait_send())
            load_tile(at, True)
            pl.when(at < PAIR * n_tiles - 1)(lambda: load_tile(at + 1, False))
            cols = tile_columns(at % n_tiles)
            inner[:, cols] = (dot(right[...], w_tile[at % PAIR], (1, 1)) * s_tile[at % PAIR]).astype(BF16)
            place = pl.ds(pl.multiple_of(t % 3 * piece_cols, piece_cols), piece_cols)
            value = dot(outer[...], inner[:, cols], (0, 0)).reshape(RING, RING, ROWS, piece_cols)
            if mine:
                acc_up[stage, t // 3, :, :, :, place] += value
            else:
                stage_up[:, :, :, place] = value
                up_piece(n).start()
            return carry

        lax.fori_loop(0, 6, tile, 0)

    load_right.wait()
    down_grad(act_three, act_three, (0, 1), False, ())
    down_grad(act_three, act_one, (0, 1), True, ())
    load_outer.wait()
    up_grad(0, False, plan["up"][:6])
    up_grad(0, True, plan["up"][6:12])
    load_next.start()
    for n in range(PHASES):
        load_wide(n).wait()
        right[:, n * piece_cols:(n + 1) * piece_cols] = dot(inner[...], w_wide[...], (1, 1)).astype(BF16)
        if n < 2:
            load_wide(n + 1).start()
    load_next.wait()
    up_grad(1, False, plan["up"][12:18])
    up_grad(1, True, plan["up"][18:])
    for i in (0, 1):
        for z in range(RING):
            down_piece(i, z).wait_send()
    down_grad(act_one, act_one, (6, 7, 8), False, plan["down"][:8])
    down_grad(act_one, None, (6, 7, 8), True, plan["down"][8:])
    for i, s in plan["end"]:
        serve(i, s)

    def total(values):
        row = lax.broadcasted_iota(jnp.int32, (8, LANES), 0)
        tile = jnp.zeros((8, LANES), F32)
        for r, value in enumerate(values):
            tile = jnp.where(row == r, value, tile)
        return tile

    def all_sum(at, tile):
        for stage, (peers, own, buf, send_s, recv_s) in enumerate((
            (first, me["x"] * 2 + core, small_one, one_send, one_recv),
            (second, me["z"] * RING + me["y"], small_two, two_send, two_recv),
        )):
            small_src[at, stage] = tile
            buf[at, own] = tile
            for t, (o, device) in enumerate(peers):
                send(functools.partial(remote, small_src.at[at, stage], buf.at[at, own], send_s.at[at, t], recv_s.at[at, own], device))
            for o, device in peers:
                remote(small_src.at[at, stage], buf.at[at, o], send_s.at[at, 0], recv_s.at[at, o], device).wait_recv()
            tile = buf[at, 0]
            for o in range(1, len(peers) + 1):
                tile = tile + buf[at, o]
        return tile

    def squares(x):
        return jnp.sum(x * x)

    def rows(kind, k):
        return (slice(None), k) if kind == "up" else (k,)

    keys = (("up", 0), ("down", 0), ("up", 1), ("down", 1))
    local_sq = functools.reduce(lambda a, b: a + b, [squares(grad[kind][k]) for kind, k in keys])
    sums = all_sum(0, total([local_sq] + [squares(master[kind][rows(kind, k)]) for kind, k in keys]))
    norm = jnp.sqrt(sums[0:1, :])
    norm_ref[...] = jnp.broadcast_to(norm, norm_ref.shape)
    clip_scale = jnp.minimum(1.0, clip_ref[0] / (norm + NORM_EPS))[:, 0:1]
    master_norm = jnp.sqrt(sums)
    local = []
    for kind, k in keys:
        avg_new, sq_new, direction = adam_direction(avg[kind][rows(kind, k)], sq[kind][rows(kind, k)], grad[kind][k], clip_scale)
        avg_out[kind][rows(kind, k)] = avg_new
        sq_out[kind][rows(kind, k)] = sq_new
        grad[kind][k] = direction
        local.append(squares(direction))
    dir_norm = jnp.sqrt(all_sum(1, total(local)))
    for r, (kind, k) in enumerate(keys):
        ratio = (master_norm[r + 1:r + 2, :] / dir_norm[r:r + 1, :])[:, 0:1]
        new = master[kind][rows(kind, k)] - rate_ref[0] * ratio * grad[kind][k]
        master_out[kind][rows(kind, k)] = new
        weight[kind][k] = new.astype(BF16)

    for i in (6, 7, 8):
        for z in range(RING):
            down_piece(i, z).wait_send()
    for n in range(9, 12):
        up_piece(n).wait_send()
    for make in sent:
        make().wait_send()


def grad_update(tensors, master, avg, sq, learn_rate, clip_norm):
    tokens, down_cols = tensors[0].shape
    up_cols = tensors[3].shape[1]
    units = column_groups(Unit, REDUCE + REDUCE_LATE, up_cols // PAIR, down_cols // PAIR)
    phases = [[(u.order[p], half_bytes(u.half_shape(p), F32)) for p in range(PHASES)] for u in units]
    slots = [(11.0, (0, 1))]
    slots += [(1.7 + (t == 11) * 8, {8: (2,), 11: (3,), 20: (4,), 23: (5,)}.get(t, ())) for t in range(24)]
    slots += [(0.6, (6, 7, 8) if t == 15 else ()) for t in range(16)]
    steps = serve_order(slots, [None] * len(units), phases, 1, 12000000.0)
    plan = dict(up=steps[1:25], down=steps[25:41], end=steps[41])
    master, avg, sq = [(up.transpose(1, 0, 2), down) for up, down in (master, avg, sq)]
    blocks = [(PAIR, 6, up_cols), (PAIR, HALF, down_cols)]
    piece = up_cols // 12
    scratch = [pltpu.VMEM((PAIR, 2, RING, RING, ROWS, up_cols // RING), F32)]
    scratch += [pltpu.VMEM(u.shape, F32) for u in units if u.kind == "down"]
    scratch += [pltpu.VMEM(u.half_shape(p), F32) for u in units for p in range(PHASES) for _ in range(SENDS)]
    scratch += [pltpu.VMEM((RING, 2, 6, u.cols), F32) for u in units if u.kind == "up"]
    scratch += [pltpu.VMEM((6 if u.kind == "up" else HALF, u.cols), F32) for u in units]
    scratch += [pltpu.VMEM(b, F32) for b in blocks]
    scratch += [pltpu.VMEM((PAIR, 2, 8, LANES), F32), pltpu.VMEM((PAIR, 8, 8, LANES), F32), pltpu.VMEM((PAIR, 16, 8, LANES), F32)]
    scratch += [pltpu.VMEM((RING, RING, RING, ROWS, down_cols // PAIR), F32), pltpu.VMEM((RING, RING, ROWS, 3 * piece), F32)]
    scratch += [pltpu.VMEM((tokens, up_cols), BF16), pltpu.VMEM((tokens, down_cols), BF16), pltpu.VMEM((tokens, down_cols), BF16)]
    scratch += [pltpu.VMEM((PAIR, piece, down_cols), BF16), pltpu.VMEM((PAIR, tokens, piece), F32)]
    scratch += [pltpu.VMEM((AHEAD, tokens, up_cols // 8), BF16), pltpu.VMEM((piece, up_cols), BF16)]
    n = len(units)
    dma = pltpu.SemaphoreType.DMA
    scratch += [dma((n, RING)), dma((n, RING)), dma((12,)), dma((12,)), dma((n * PHASES * SENDS,)), dma((n * PHASES * SENDS,)), dma((n,)), dma((n,))]
    scratch += [dma((PAIR, 16)), dma((PAIR, 16)), dma((PAIR, 16)), dma((PAIR, 16)), dma((PAIR,)), dma((PAIR,)), dma((AHEAD,)), dma((PHASES,))]
    vmem, smem, any_space = [pl.BlockSpec(memory_space=s) for s in (pltpu.VMEM, pltpu.SMEM, pl.ANY)]
    state = [jax.ShapeDtypeStruct(a.shape, F32) for a in master]
    return pl.pallas_call(
        functools.partial(grad_update_kernel, units, plan),
        out_shape=[jax.ShapeDtypeStruct(b, BF16) for b in blocks] + state * 3 + [jax.ShapeDtypeStruct((8, LANES), F32)],
        in_specs=[any_space] * len(tensors) + [vmem] * 6 + [smem] * 2,
        out_specs=[vmem] * 9,
        scratch_shapes=scratch,
        compiler_params=pltpu.CompilerParams(collective_id=0, has_side_effects=True, vmem_limit_bytes=FULL_VMEM),
        name="grad_update",
    )(*tensors, *master, *avg, *sq, learn_rate.reshape(1), clip_norm.reshape(1))


class Gather:
    def __init__(self, kind, k, off, cols, order):
        self.kind, self.k, self.off, self.cols, self.order = kind, k, off, cols, order
        self.dims = "zy" if kind == "up" else "zyx"
        self.shape = (RING,) * len(self.dims) + (ROWS, cols)

    def chunk(self, phase, owner, me, h=None):
        gathered, d = self.order[:phase], self.order[phase]
        index, shape, split = [], [], h is None
        for e in self.dims:
            if e == d:
                index.append(owner)
            elif e not in gathered:
                index.append(me[e])
            elif split:
                index.append(slice(None))
                shape.append(RING)
            else:
                index.append(pl.ds(PAIR * h, 2))
                shape.append(2)
                split = True
        if split:
            return tuple(index), tuple(shape) + (ROWS, self.cols)
        return tuple(index) + (pl.ds(HALF * h, HALF),), (HALF, self.cols)


def gather_kernel(units, events, up_ref, down_ref, out_up, out_down, *refs):
    take = iter(refs)
    block = [next(take) for _ in units]
    rows_up, rows_down, assembly = next(take), next(take), next(take)
    row_send, row_recv, core_send, core_recv, ring_send, ring_recv, own_sem, share_send, share_recv = [next(take) for _ in range(9)]
    me = position()
    core = me["c"]
    partner = partner_of(me)
    own = me["x"] * 2 + core
    first = group_peers(me)[0]
    around = [moved(me, d, by) for d in "zy" for by in (1, -1)]
    half_up, half_down = up_ref.shape[-1] // PAIR, down_ref.shape[-1] // PAIR

    barrier = pltpu.get_barrier_semaphore()
    for device in [device for _, device in first] + around:
        pl.semaphore_signal(barrier, inc=1, device_id=device, device_id_type=MESH)
    pl.semaphore_wait(barrier, len(first) + len(around))

    sent = []

    def send(copy):
        copy.start()
        sent.append(copy)

    other = pl.ds(pl.multiple_of((1 - core) * half_down, LANES), half_down)
    core_copy = remote(down_ref.at[:, :, other], rows_down, core_send, core_recv, partner)
    send(core_copy)
    for t, (o, device) in enumerate(first):
        width = pl.ds(pl.multiple_of((o % PAIR) * half_up, LANES), half_up)
        send(remote(up_ref.at[:, :, width], rows_up.at[own], row_send.at[t], row_recv.at[own], device))

    def part(i, phase, owner, h=None, of=core):
        u = units[i]
        out, half = (out_up, half_up) if u.kind == "up" else (out_down, half_down)
        at = u.chunk(phase, owner, me, h)[0]
        at = at + (slice(None),) * (len(u.dims) + 1 - len(at))
        return out.at[(u.k,) + at + (pl.ds(pl.multiple_of(of * half + u.off, LANES), u.cols),)]

    def ring(i, phase, n):
        d = units[i].order[phase]
        by = 1 if n % PAIR == 0 else -1
        owner = me[d] if n < 4 else (me[d] - by) % RING
        ref = part(i, phase, owner, (0, 1, 1, 0, 0, 1)[n])
        s = (i * PHASES + phase) * SENDS + n
        return remote(ref, ref, ring_send.at[s], ring_recv.at[s], moved(me, d, by))

    def start_phase(i, phase):
        for n in range(4):
            send(ring(i, phase, n))

    shares = []

    def share(i, j, owner):
        phase = len(units[i].order) - 1
        mine, theirs = part(i, phase, owner), part(i, phase, owner, None, 1 - core)
        send(remote(mine, mine, share_send.at[i, j], share_recv.at[i, j], partner))
        shares.append(remote(theirs, theirs, share_send.at[i, j], share_recv.at[i, j], partner))

    rows_ready = [False]
    for i, s in events:
        u = units[i]
        last = len(u.order) - 1
        if s == 0:
            if u.kind == "down":
                if i == 0:
                    core_copy.wait_recv()
                low, high = down_ref[u.k, :, u.off:u.off + u.cols], down_ref[u.k, :, half_down + u.off:half_down + u.off + u.cols]
                mine = jnp.where(core == 0, low, high)
                theirs = rows_down[u.k, :, u.off:u.off + u.cols]
                block[i][...] = jnp.concatenate([jnp.where(core == 0, mine, theirs), jnp.where(core == 0, theirs, mine)], axis=0)
            else:
                if not rows_ready[0]:
                    rows_ready[0] = True
                    rows_up[own] = jnp.where(core == 0, up_ref[:, :, :half_up], up_ref[:, :, half_up:])
                    for o, device in first:
                        remote(rows_up.at[o], rows_up.at[o], row_send.at[0], row_recv.at[o], device).wait_recv()
                for p in range(8):
                    assembly[6 * p:6 * p + 6, :] = rows_up[p, u.k, :, u.off:u.off + u.cols].astype(F32)
                block[i][...] = assembly[...].astype(BF16)
            own_copy = pltpu.make_async_copy(block[i], part(i, 0, me[u.order[0]]), own_sem.at[i])
            own_copy.start()
            own_copy.wait()
            start_phase(i, 0)
        elif s % PAIR == 1:
            phase = (s - 1) // PAIR
            if phase == last:
                share(i, 0, me[u.order[last]])
            for n in (4, 5):
                d = u.order[phase]
                incoming = part(i, phase, (me[d] + (-1 if n == 4 else 1)) % RING, n - 4)
                remote(incoming, incoming, ring_send.at[0], ring_recv.at[(i * PHASES + phase) * SENDS + n - 4], moved(me, d, 1)).wait_recv()
                send(ring(i, phase, n))
        else:
            phase = s // PAIR - 1
            d = u.order[phase]
            for n in (PAIR, 3, 4, 5):
                step = {2: -1, 3: 1, 4: -2, 5: 2}[n]
                h = {2: 1, 3: 0, 4: 0, 5: 1}[n]
                incoming = part(i, phase, (me[d] + step) % RING, h)
                remote(incoming, incoming, ring_send.at[0], ring_recv.at[(i * PHASES + phase) * SENDS + n], moved(me, d, 1)).wait_recv()
                if phase == last and n == 3:
                    share(i, 1, (me[d] - 1) % RING)
                    share(i, 2, (me[d] + 1) % RING)
            if phase < last:
                start_phase(i, phase + 1)
            else:
                share(i, 3, (me[d] + 2) % RING)

    for copy in shares:
        copy.wait_recv()
    for copy in sent:
        copy.wait_send()


def gather_weights(block_up, block_down):
    up_cols, down_cols = block_up.shape[2], block_down.shape[2]
    units = column_groups(Gather, GATHER + GATHER_LATE, up_cols // PAIR, down_cols // PAIR)
    here = dict(x=0, y=0, z=0)
    phases = [[(d, half_bytes(u.chunk(p, 0, here, 0)[1], BF16)) for p, d in enumerate(u.order)] for u in units]
    events = serve_order((), [2.0 if u.kind == "down" else 6.0 for u in units], phases, 0, math.inf)[0]
    n = len(units)
    dma = pltpu.SemaphoreType.DMA
    scratch = [pltpu.VMEM((ROWS, u.cols), BF16) for u in units]
    scratch += [pltpu.VMEM((8, 2, 6, up_cols // PAIR), BF16), pltpu.VMEM((PAIR, HALF, down_cols // PAIR), BF16), pltpu.VMEM((ROWS, up_cols // 4), F32)]
    scratch += [dma((7,)), dma((8,)), dma, dma, dma((n * PHASES * SENDS,)), dma((n * PHASES * SENDS,)), dma((n,)), dma((n, 4)), dma((n, 4))]
    vmem = pl.BlockSpec(memory_space=pltpu.VMEM)
    out_up, out_down = pl.pallas_call(
        functools.partial(gather_kernel, units, events),
        out_shape=[jax.ShapeDtypeStruct((PAIR, RING, RING, ROWS, up_cols), BF16), jax.ShapeDtypeStruct((PAIR, RING, RING, RING, ROWS, down_cols), BF16)],
        in_specs=[vmem] * 2,
        out_specs=[pl.BlockSpec(memory_space=pl.ANY)] * 2,
        scratch_shapes=scratch,
        compiler_params=pltpu.CompilerParams(collective_id=1, has_side_effects=True, vmem_limit_bytes=HALF * 1024 * 1024),
        name="gather_weights",
    )(block_up, block_down)
    return out_up, out_down


def finish_weights_kernel(up, down, out_up, out_down, sems):
    copies = [pltpu.make_async_copy(src.at[k, z], dst.at[k, z], sems.at[i, k, z]) for i, (src, dst) in enumerate(((up, out_up), (down, out_down))) for k in range(PAIR) for z in range(RING)]
    for copy in copies:
        copy.start()
    for copy in copies:
        copy.wait()


def finish_state_kernel(*refs):
    n = len(refs) // 3
    into = [pltpu.make_async_copy(src, buf, refs[-1].at[i]) for i, (src, buf) in enumerate(zip(refs[:n], refs[PAIR * n:-1]))]
    back = [pltpu.make_async_copy(buf, dst, refs[-1].at[i]) for i, (buf, dst) in enumerate(zip(refs[PAIR * n:-1], refs[n:]))]
    for copy in into:
        copy.start()
    for one, other in zip(into, back):
        one.wait()
        other.start()
    for copy in back:
        copy.wait()


def finish(kernel, arrays, scratch, limit):
    any_space = pl.BlockSpec(memory_space=pl.ANY)
    return pl.pallas_call(
        kernel,
        out_shape=[jax.ShapeDtypeStruct(a.shape, a.dtype) for a in arrays],
        in_specs=[any_space] * len(arrays),
        out_specs=[any_space] * len(arrays),
        scratch_shapes=scratch,
        compiler_params=pltpu.CompilerParams(vmem_limit_bytes=limit),
    )(*arrays)


def solution(mesh):
    batch_rows = P("data", None)
    state_rows = P(None, "data", None)
    replicated = P()

    def device_step(act_in, grad_out, w_up, w_down, master_up, master_down, exp_avg_up, exp_avg_down, exp_sq_up, exp_sq_down, learn_rate, clip_norm):
        act_one, slope_one, hidden, act_three, slope_three = forward(act_in, w_up, w_down)
        tensors = (act_in, grad_out, hidden, act_one, act_three, slope_one, slope_three, w_up, w_down)
        outs = grad_update(tensors, (master_up, master_down), (exp_avg_up, exp_avg_down), (exp_sq_up, exp_sq_down), learn_rate, clip_norm)
        dma = pltpu.SemaphoreType.DMA
        small = [pltpu.VMEM(a.shape, F32) for a in outs[2:]]
        *state, norm = finish(finish_state_kernel, outs[2:], small + [dma((len(small),))], FULL_VMEM)
        new_w_up, new_w_down = finish(finish_weights_kernel, gather_weights(*outs[:2]), [dma((PAIR, PAIR, RING))], WEIGHT_LIMIT)
        state = [a.transpose(1, 0, 2) if i % PAIR == 0 else a for i, a in enumerate(state)]
        return (new_w_up.reshape(w_up.shape), new_w_down.reshape(w_down.shape), *state, norm[0, 0])

    return jax.shard_map(device_step, mesh=mesh, in_specs=(batch_rows, batch_rows, replicated, replicated, state_rows, state_rows, state_rows, state_rows, state_rows, state_rows, replicated, replicated), out_specs=(replicated, replicated, state_rows, state_rows, state_rows, state_rows, state_rows, state_rows, replicated), check_vma=False)
```

```python
import functools
import math

import jax
import jax.numpy as jnp
from jax import lax
from jax.experimental import pallas as pl
from jax.experimental.pallas import tpu as pltpu
from jax.sharding import PartitionSpec as P

STEP = 10
BETA_ONE = 0.9
BETA_TWO = 0.95
ADAM_EPS = 1e-8
NORM_EPS = 1e-6
INV_SQRT_TWO = 0.7071067811865476
INV_SQRT_TWO_PI = 0.3989422804014327

MESH = pl.DeviceIdType.MESH
RING = 4
ROWS = 48
HALF = 24
LANES = 128
PAIR = 2
PHASES = 3
FULL_VMEM = 67043328
WEIGHT_LIMIT = 4194304
AHEAD = 4
SENDS = 6
F32 = jnp.float32
BF16 = jnp.bfloat16


def gelu_parts(pre_act):
    normal_cdf = 0.5 * (1.0 + lax.erf(pre_act * INV_SQRT_TWO))
    normal_pdf = jnp.exp(-0.5 * pre_act * pre_act) * INV_SQRT_TWO_PI
    return pre_act * normal_cdf, normal_cdf + pre_act * normal_pdf


def forward(act_in, w_up, w_down):
    z_one = jnp.einsum("td,df->tf", act_in, w_up[0], preferred_element_type=jnp.float32)
    gelu_one, slope_one = gelu_parts(z_one)
    act_one = gelu_one.astype(jnp.bfloat16)
    hidden = jnp.einsum("tf,fd->td", act_one, w_down[0], preferred_element_type=jnp.float32).astype(jnp.bfloat16)
    z_three = jnp.einsum("td,df->tf", hidden, w_up[1], preferred_element_type=jnp.float32)
    gelu_three, slope_three = gelu_parts(z_three)
    return act_one, slope_one, hidden, gelu_three.astype(jnp.bfloat16), slope_three


def adam_direction(exp_avg, exp_sq, grad, clip_scale):
    bias_one = 1.0 - BETA_ONE ** STEP
    bias_two = 1.0 - BETA_TWO ** STEP
    avg_new = BETA_ONE * exp_avg + (1.0 - BETA_ONE) * clip_scale * grad
    sq_new = BETA_TWO * exp_sq + (1.0 - BETA_TWO) * (clip_scale * clip_scale) * (grad * grad)
    direction = (avg_new / bias_one) / (jnp.sqrt(sq_new / bias_two) + ADAM_EPS)
    return avg_new, sq_new, direction


class Unit:
    def __init__(self, kind, k, off, cols, order):
        self.kind, self.k, self.off, self.cols, self.order = kind, k, off, cols, order
        self.dims = "zy" if kind == "up" else "zyx"
        self.shape = (RING,) * len(self.dims) + (ROWS, cols)

    def half(self, phase, dest, h, me):
        if self.kind == "up" and phase == 2:
            return (dest, h), (6, self.cols)
        fixed = {d: me[d] for d in self.order[:phase]}
        fixed[self.order[phase]] = dest
        index, shape, split = [], [], False
        for d in self.dims:
            if d in fixed:
                index.append(fixed[d])
            elif not split:
                index.append(pl.ds(PAIR * h, 2))
                shape.append(2)
                split = True
            else:
                index.append(slice(None))
                shape.append(RING)
        if split:
            return tuple(index), tuple(shape) + (ROWS, self.cols)
        return tuple(index) + (pl.ds(HALF * h, HALF),), (HALF, self.cols)

    def half_shape(self, phase):
        return self.half(phase, 0, 0, dict(x=0, y=0, z=0))[1]


def column_groups(make, specs, up_cols, down_cols):
    groups = []
    for spec in specs:
        k, first, count = map(int, spec[1:4])
        kind, part = ("up", up_cols // PAIR) if spec[0] == "u" else ("down", down_cols // 3)
        groups.append(make(kind, k, first * part, count * part, spec[4:]))
    return groups


REDUCE = ("d102xzy", "d121xzy", "u101zyx", "u111yzx")
REDUCE_LATE = ("u001zyx", "u011yzx", "d001xzy", "d011xzy", "d021xyz")
GATHER = ("d102zyx", "d002yzx", "d121xzy", "d021xyz")
GATHER_LATE = ("u101yz", "u111zy", "u001yz", "u011zy")


def serve_order(slots, ready, phases, tail, moved_per_us):
    rate, hop = 44000.0, 3.0
    link, now, plan = {}, 0.0, []
    ready, state, late = list(ready), [0] * len(ready), [0.0] * len(ready)
    ends = [PAIR * len(p) + tail for p in phases]

    def send(phase):
        d, nbytes = phase
        for sign in "+-":
            link[d, sign] = max(link.get((d, sign), 0.0), now) + nbytes / rate
        return max(link[d, sign] for sign in "+-") + hop

    for duration, starts in list(slots) + [(None, ())]:
        served = []
        while True:
            open_units = [j for j in range(len(ready)) if state[j] <= ends[j] and ready[j] is not None]
            if not open_units:
                break
            i = min(open_units, key=lambda j: (ready[j], j))
            if duration is not None and ready[i] > now:
                break
            phase, middle = divmod(state[i], 2)
            served.append((i, state[i]))
            now = max(now, ready[i])
            if state[i]:
                now += 0.05 + 8 * phases[i][(state[i] - 1) // PAIR if state[i] <= PAIR * len(phases[i]) else -1][1] / moved_per_us
            if phase < len(phases[i]):
                ready[i] = send(phases[i][phase])
                if middle:
                    ready[i] = max(ready[i], late[i])
                else:
                    late[i] = send(phases[i][phase])
            else:
                ready[i] = now + hop
            state[i] += 1
        plan.append(served)
        if duration is not None:
            now += duration
            for i in starts:
                ready[i] = now
    return plan


def half_bytes(shape, dtype):
    return math.prod(shape) * jnp.dtype(dtype).itemsize


def position():
    me = lax.axis_index("data")
    return dict(z=me // 32, y=(me // 8) % RING, x=(me // PAIR) % RING, c=me % PAIR)


def device_of(at):
    return (((at["z"] * RING + at["y"]) * RING + at["x"]) * 2 + at["c"],)


def moved(me, d, by):
    return device_of({**me, d: (me[d] + by) % RING})


def partner_of(me):
    return device_of({**me, "c": 1 - me["c"]})


def group_peers(me):
    first, second = [], []
    j, q = me["x"] * 2 + me["c"], me["z"] * 4 + me["y"]
    for t in range(1, 8):
        o = (j + t) % 8
        first.append((o, device_of({**me, "x": o // PAIR, "c": o % PAIR})))
    for t in range(1, 16):
        o = (q + t) % 16
        second.append((o, device_of({**me, "z": o // 4, "y": o % RING})))
    return first, second


def remote(src, dst, send_sem, recv_sem, device):
    return pltpu.make_async_remote_copy(src_ref=src, dst_ref=dst, send_sem=send_sem, recv_sem=recv_sem, device_id=device, device_id_type=MESH)


def add_into(dst, *srcs):
    lead = dst.shape[:-2]
    if not lead:
        dst[...] = functools.reduce(lambda a, b: a + b, [s[...] for s in srcs], dst[...])
        return

    def body(i, carry):
        index = []
        for n in reversed(lead):
            index.append(i % n)
            i = i // n
        index = tuple(reversed(index))
        dst[index] = functools.reduce(lambda a, b: a + b, [s[index] for s in srcs], dst[index])
        return carry

    lax.fori_loop(0, math.prod(lead), body, 0)


def dot(a, b, contract):
    return lax.dot_general(a, b, ((contract[:1], contract[1:]), ((), ())), preferred_element_type=F32)


def grad_update_kernel(units, plan, *refs):
    take = iter(refs)
    act_in, grad_out, hidden, act_one, act_three, slope_one, slope_three, w_up, w_down = [next(take) for _ in range(9)]
    master = dict(up=next(take), down=next(take))
    avg = dict(up=next(take), down=next(take))
    sq = dict(up=next(take), down=next(take))
    rate_ref, clip_ref = next(take), next(take)
    weight = dict(up=next(take), down=next(take))
    master_out = dict(up=next(take), down=next(take))
    avg_out = dict(up=next(take), down=next(take))
    sq_out = dict(up=next(take), down=next(take))
    norm_ref = next(take)
    acc_up = next(take)
    acc = [acc_up.at[1 - u.k, int(u.off > 0)] if u.kind == "up" else next(take) for u in units]
    recv = [[[next(take) for _ in range(SENDS)] for _ in range(PHASES)] for _ in units]
    xbuf = {i: next(take) for i, u in enumerate(units) if u.kind == "up"}
    fin = [next(take) for _ in units]
    grad = dict(up=next(take), down=next(take))
    small_src, small_one, small_two = next(take), next(take), next(take)
    stage_down, stage_up, inner, right, outer, w_tile, s_tile, a_tile, w_wide = [next(take) for _ in range(9)]
    down_send, down_recv, up_send, up_recv, ring_send, ring_recv, fin_send, fin_recv = [next(take) for _ in range(8)]
    one_send, one_recv, two_send, two_recv = [next(take) for _ in range(4)]
    w_sem, s_sem, a_sem, load_sem = [next(take) for _ in range(4)]

    me = position()
    core = me["c"]
    partner = partner_of(me)
    first, second = group_peers(me)
    n_tiles, piece_cols, wide = 12, w_tile.shape[1], a_tile.shape[2]
    down_half = grad["down"].shape[-1] // PAIR

    load_right = pltpu.make_async_copy(grad_out, right, load_sem.at[0])
    load_outer = pltpu.make_async_copy(hidden, outer, load_sem.at[1])
    load_next = pltpu.make_async_copy(act_in, outer, load_sem.at[1])

    def load_wide(n):
        rows = pl.ds(pl.multiple_of(n * piece_cols, piece_cols), piece_cols)
        return pltpu.make_async_copy(w_up.at[1, rows], w_wide, load_sem.at[2])

    def load_a(source, t):
        return pltpu.make_async_copy(source.at[:, pl.ds(pl.multiple_of(t % 8 * wide, LANES), wide)], a_tile.at[t % AHEAD], a_sem.at[t % AHEAD])

    def tile_columns(t):
        half = jnp.where(t < n_tiles // PAIR, 1 - core, core)
        return pl.ds(pl.multiple_of((half * (n_tiles // PAIR) + t % (n_tiles // PAIR)) * piece_cols, piece_cols), piece_cols)

    def load_tile(at, wait):
        stage, slot, cols = at // n_tiles, at % PAIR, tile_columns(at % n_tiles)
        w_copy = pltpu.make_async_copy(w_down.at[1 - stage, cols], w_tile.at[slot], w_sem.at[slot])
        if wait:
            w_copy.wait()
            pltpu.make_async_copy(slope_one.at[:, cols], s_tile.at[slot], s_sem.at[slot]).wait()
            return
        w_copy.start()
        for n, source in enumerate((slope_three, slope_one)):
            pl.when(stage == n)(pltpu.make_async_copy(source.at[:, cols], s_tile.at[slot], s_sem.at[slot]).start)

    load_right.start()
    for t in range(AHEAD - 1):
        load_a(act_three, t).start()
    load_outer.start()
    load_tile(0, False)
    load_wide(0).start()

    barrier = pltpu.get_barrier_semaphore()
    for _, device in first + second:
        pl.semaphore_signal(barrier, inc=1, device_id=device, device_id_type=MESH)
    pl.semaphore_wait(barrier, len(first) + len(second))

    sent = []

    def ring(i, phase, n):
        u = units[i]
        d = u.order[phase]
        base = xbuf[i] if u.kind == "up" and phase == 2 else acc[i]
        by = 1 if n % PAIR == 0 else -1
        dest = (me[d] + (2 if n < 2 else by)) % RING
        h = (0, 1, 1, 0, 0, 1)[n]
        src = base.at[u.half(phase, dest, h, me)[0]]
        s = (i * PHASES + phase) * SENDS + n
        return remote(src, recv[i][phase][n], ring_send.at[s], ring_recv.at[s], moved(me, d, by))

    def last_piece(i, c):
        u = units[i]
        if u.kind == "up":
            return xbuf[i].at[me["x"], c]
        return acc[i].at[me["z"], me["y"], me["x"], pl.ds(pl.multiple_of(HALF * c, 8), HALF)]

    def swap(i):
        return remote(last_piece(i, 1 - core), fin[i], fin_send.at[i], fin_recv.at[i], partner)

    def send(make):
        make().start()
        sent.append(make)

    def start_phase(i, phase):
        u = units[i]
        if u.kind == "up" and phase == 2:
            block = acc[i][me["z"], me["y"]]
            for p in range(8):
                xbuf[i][p // PAIR, p % PAIR] = block[6 * p:6 * p + 6]
        for n in range(4):
            send(functools.partial(ring, i, phase, n))

    def serve(i, s):
        u = units[i]
        if s == 0:
            start_phase(i, 0)
        elif s < 7 and s % PAIR == 1:
            phase = (s - 1) // PAIR
            d = u.order[phase]
            base = xbuf[i] if u.kind == "up" and phase == 2 else acc[i]
            for n in (4, 5):
                ring(i, phase, n - 4).wait_recv()
                dest = (me[d] + (1 if n == 4 else -1)) % RING
                add_into(base.at[u.half(phase, dest, n - 4, me)[0]], recv[i][phase][n - 4])
                send(functools.partial(ring, i, phase, n))
        elif s < 7:
            phase = s // PAIR - 1
            d = u.order[phase]
            base = xbuf[i] if u.kind == "up" and phase == 2 else acc[i]
            for n in (PAIR, 3, 4, 5):
                ring(i, phase, n).wait_recv()
            for h, (a, b) in enumerate(((4, 3), (PAIR, 5))):
                add_into(base.at[u.half(phase, me[d], h, me)[0]], recv[i][phase][a], recv[i][phase][b])
            if phase < 2:
                start_phase(i, phase + 1)
            else:
                send(functools.partial(swap, i))
        else:
            swap(i).wait_recv()
            own, other = last_piece(i, core)[...], fin[i][...]
            half = grad[u.kind].shape[-1] // PAIR
            grad[u.kind][u.k, :, u.off:u.off + u.cols] = jnp.where(core == 0, own, other) * (1.0 / 128.0)
            grad[u.kind][u.k, :, half + u.off:half + u.off + u.cols] = jnp.where(core == 0, other, own) * (1.0 / 128.0)

    def serve_at(t, steps):
        if steps:
            @pl.when(t[0] == t[1])
            def _():
                for i, s in steps:
                    serve(i, s)

    def down_piece(i, z):
        u = units[i]
        return remote(stage_down.at[z, :, :, :, u.off:u.off + u.cols], acc[i].at[z], down_send.at[i, z], down_recv.at[i, z], partner)

    def down_grad(source, following, group, mine, steps):
        columns = core if mine else 1 - core

        def tile(t, carry):
            for k, served in enumerate(steps):
                serve_at((t, k), served)
            z, y = t // PAIR, pl.ds(t % PAIR * 2, 2)
            if mine:
                pl.when(t % PAIR == 0)(lambda: [down_piece(i, z).wait_recv() for i in group] and None)
            load_a(source, t).wait()
            later = t + AHEAD - 1
            pl.when(later < 8)(lambda: load_a(source, later).start())
            if following is not None:
                pl.when(later >= 8)(lambda: load_a(following, later).start())
            value = dot(a_tile[t % AHEAD], right[:, pl.ds(pl.multiple_of(columns * down_half, LANES), down_half)], (0, 0))
            value = value.reshape(PAIR, RING, ROWS, down_half)
            if mine:
                for i in group:
                    acc[i][z, y] += value[..., units[i].off:units[i].off + units[i].cols]
            else:
                stage_down[z, y] = value
                pl.when(t % PAIR == 1)(lambda: [down_piece(i, z).start() for i in group] and None)
            return carry

        lax.fori_loop(0, 8, tile, 0)

    def up_piece(n):
        cols = pl.ds(pl.multiple_of(n % 3 * piece_cols, piece_cols), piece_cols)
        return remote(stage_up.at[:, :, :, cols], acc_up.at[n // 6, n // 3 % PAIR, :, :, :, cols], up_send.at[n], up_recv.at[n], partner)

    def up_grad(stage, mine, steps):
        start = stage * n_tiles + mine * 6

        def tile(t, carry):
            for k, served in enumerate(steps):
                serve_at((t, k), served)
            at = start + t
            n = stage * 6 + t
            if mine:
                up_piece(n).wait_recv()
            else:
                pl.when(n > 2)(lambda: up_piece(n - 3).wait_send())
            load_tile(at, True)
            pl.when(at < PAIR * n_tiles - 1)(lambda: load_tile(at + 1, False))
            cols = tile_columns(at % n_tiles)
            inner[:, cols] = (dot(right[...], w_tile[at % PAIR], (1, 1)) * s_tile[at % PAIR]).astype(BF16)
            place = pl.ds(pl.multiple_of(t % 3 * piece_cols, piece_cols), piece_cols)
            value = dot(outer[...], inner[:, cols], (0, 0)).reshape(RING, RING, ROWS, piece_cols)
            if mine:
                acc_up[stage, t // 3, :, :, :, place] += value
            else:
                stage_up[:, :, :, place] = value
                up_piece(n).start()
            return carry

        lax.fori_loop(0, 6, tile, 0)

    load_right.wait()
    down_grad(act_three, act_three, (0, 1), False, ())
    down_grad(act_three, act_one, (0, 1), True, ())
    load_outer.wait()
    up_grad(0, False, plan["up"][:6])
    up_grad(0, True, plan["up"][6:12])
    load_next.start()
    for n in range(PHASES):
        load_wide(n).wait()
        right[:, n * piece_cols:(n + 1) * piece_cols] = dot(inner[...], w_wide[...], (1, 1)).astype(BF16)
        if n < 2:
            load_wide(n + 1).start()
    load_next.wait()
    for i in (0, 1):
        for z in range(RING):
            down_piece(i, z).wait_send()
    down_grad(act_one, act_one, (6, 7, 8), False, plan["down"][:8])
    down_grad(act_one, None, (6, 7, 8), True, plan["down"][8:])
    up_grad(1, False, plan["up"][12:18])
    up_grad(1, True, plan["up"][18:])
    for i, s in plan["end"]:
        serve(i, s)

    def total(values):
        row = lax.broadcasted_iota(jnp.int32, (8, LANES), 0)
        tile = jnp.zeros((8, LANES), F32)
        for r, value in enumerate(values):
            tile = jnp.where(row == r, value, tile)
        return tile

    def all_sum(at, tile):
        for stage, (peers, own, buf, send_s, recv_s) in enumerate((
            (first, me["x"] * 2 + core, small_one, one_send, one_recv),
            (second, me["z"] * RING + me["y"], small_two, two_send, two_recv),
        )):
            small_src[at, stage] = tile
            buf[at, own] = tile
            for t, (o, device) in enumerate(peers):
                send(functools.partial(remote, small_src.at[at, stage], buf.at[at, own], send_s.at[at, t], recv_s.at[at, own], device))
            for o, device in peers:
                remote(small_src.at[at, stage], buf.at[at, o], send_s.at[at, 0], recv_s.at[at, o], device).wait_recv()
            tile = buf[at, 0]
            for o in range(1, len(peers) + 1):
                tile = tile + buf[at, o]
        return tile

    def squares(x):
        return jnp.sum(x * x)

    def rows(kind, k):
        return (slice(None), k) if kind == "up" else (k,)

    keys = (("up", 0), ("down", 0), ("up", 1), ("down", 1))
    local_sq = functools.reduce(lambda a, b: a + b, [squares(grad[kind][k]) for kind, k in keys])
    sums = all_sum(0, total([local_sq] + [squares(master[kind][rows(kind, k)]) for kind, k in keys]))
    norm = jnp.sqrt(sums[0:1, :])
    norm_ref[...] = jnp.broadcast_to(norm, norm_ref.shape)
    clip_scale = jnp.minimum(1.0, clip_ref[0] / (norm + NORM_EPS))[:, 0:1]
    master_norm = jnp.sqrt(sums)
    local = []
    for kind, k in keys:
        avg_new, sq_new, direction = adam_direction(avg[kind][rows(kind, k)], sq[kind][rows(kind, k)], grad[kind][k], clip_scale)
        avg_out[kind][rows(kind, k)] = avg_new
        sq_out[kind][rows(kind, k)] = sq_new
        grad[kind][k] = direction
        local.append(squares(direction))
    dir_norm = jnp.sqrt(all_sum(1, total(local)))
    for r, (kind, k) in enumerate(keys):
        ratio = (master_norm[r + 1:r + 2, :] / dir_norm[r:r + 1, :])[:, 0:1]
        new = master[kind][rows(kind, k)] - rate_ref[0] * ratio * grad[kind][k]
        master_out[kind][rows(kind, k)] = new
        weight[kind][k] = new.astype(BF16)

    for i in (6, 7, 8):
        for z in range(RING):
            down_piece(i, z).wait_send()
    for n in range(9, 12):
        up_piece(n).wait_send()
    for make in sent:
        make().wait_send()


def grad_update(tensors, master, avg, sq, learn_rate, clip_norm):
    tokens, down_cols = tensors[0].shape
    up_cols = tensors[3].shape[1]
    units = column_groups(Unit, REDUCE + REDUCE_LATE, up_cols // PAIR, down_cols // PAIR)
    phases = [[(u.order[p], half_bytes(u.half_shape(p), F32)) for p in range(PHASES)] for u in units]
    slots = [(11.0, (0, 1))] + [(1.7 + (t == 11) * 8, {8: (2,), 11: (3,)}.get(t, ())) for t in range(12)]
    slots += [(0.6, (6, 7, 8) if t == 15 else ()) for t in range(16)] + [(1.7, {8: (4,), 11: (5,)}.get(t, ())) for t in range(12)]
    steps = serve_order(slots, [None] * len(units), phases, 1, 12000000.0)
    plan = dict(up=steps[1:13] + steps[29:41], down=steps[13:29], end=steps[41])
    master, avg, sq = [(up.transpose(1, 0, 2), down) for up, down in (master, avg, sq)]
    blocks = [(PAIR, 6, up_cols), (PAIR, HALF, down_cols)]
    piece = up_cols // 12
    scratch = [pltpu.VMEM((PAIR, 2, RING, RING, ROWS, up_cols // RING), F32)]
    scratch += [pltpu.VMEM(u.shape, F32) for u in units if u.kind == "down"]
    scratch += [pltpu.VMEM(u.half_shape(p), F32) for u in units for p in range(PHASES) for _ in range(SENDS)]
    scratch += [pltpu.VMEM((RING, 2, 6, u.cols), F32) for u in units if u.kind == "up"]
    scratch += [pltpu.VMEM((6 if u.kind == "up" else HALF, u.cols), F32) for u in units]
    scratch += [pltpu.VMEM(b, F32) for b in blocks]
    scratch += [pltpu.VMEM((PAIR, 2, 8, LANES), F32), pltpu.VMEM((PAIR, 8, 8, LANES), F32), pltpu.VMEM((PAIR, 16, 8, LANES), F32)]
    scratch += [pltpu.VMEM((RING, RING, RING, ROWS, down_cols // PAIR), F32), pltpu.VMEM((RING, RING, ROWS, 3 * piece), F32)]
    scratch += [pltpu.VMEM((tokens, up_cols), BF16), pltpu.VMEM((tokens, down_cols), BF16), pltpu.VMEM((tokens, down_cols), BF16)]
    scratch += [pltpu.VMEM((PAIR, piece, down_cols), BF16), pltpu.VMEM((PAIR, tokens, piece), F32)]
    scratch += [pltpu.VMEM((AHEAD, tokens, up_cols // 8), BF16), pltpu.VMEM((piece, up_cols), BF16)]
    n = len(units)
    dma = pltpu.SemaphoreType.DMA
    scratch += [dma((n, RING)), dma((n, RING)), dma((12,)), dma((12,)), dma((n * PHASES * SENDS,)), dma((n * PHASES * SENDS,)), dma((n,)), dma((n,))]
    scratch += [dma((PAIR, 16)), dma((PAIR, 16)), dma((PAIR, 16)), dma((PAIR, 16)), dma((PAIR,)), dma((PAIR,)), dma((AHEAD,)), dma((PHASES,))]
    vmem, smem, any_space = [pl.BlockSpec(memory_space=s) for s in (pltpu.VMEM, pltpu.SMEM, pl.ANY)]
    state = [jax.ShapeDtypeStruct(a.shape, F32) for a in master]
    return pl.pallas_call(
        functools.partial(grad_update_kernel, units, plan),
        out_shape=[jax.ShapeDtypeStruct(b, BF16) for b in blocks] + state * 3 + [jax.ShapeDtypeStruct((8, LANES), F32)],
        in_specs=[any_space] * len(tensors) + [vmem] * 6 + [smem] * 2,
        out_specs=[vmem] * 9,
        scratch_shapes=scratch,
        compiler_params=pltpu.CompilerParams(collective_id=0, has_side_effects=True, vmem_limit_bytes=FULL_VMEM),
        name="grad_update",
    )(*tensors, *master, *avg, *sq, learn_rate.reshape(1), clip_norm.reshape(1))


class Gather:
    def __init__(self, kind, k, off, cols, order):
        self.kind, self.k, self.off, self.cols, self.order = kind, k, off, cols, order
        self.dims = "zy" if kind == "up" else "zyx"
        self.shape = (RING,) * len(self.dims) + (ROWS, cols)

    def chunk(self, phase, owner, me, h=None):
        gathered, d = self.order[:phase], self.order[phase]
        index, shape, split = [], [], h is None
        for e in self.dims:
            if e == d:
                index.append(owner)
            elif e not in gathered:
                index.append(me[e])
            elif split:
                index.append(slice(None))
                shape.append(RING)
            else:
                index.append(pl.ds(PAIR * h, 2))
                shape.append(2)
                split = True
        if split:
            return tuple(index), tuple(shape) + (ROWS, self.cols)
        return tuple(index) + (pl.ds(HALF * h, HALF),), (HALF, self.cols)


def gather_kernel(units, events, up_ref, down_ref, out_up, out_down, *refs):
    take = iter(refs)
    block = [next(take) for _ in units]
    rows_up, rows_down, assembly = next(take), next(take), next(take)
    row_send, row_recv, core_send, core_recv, ring_send, ring_recv, own_sem, share_send, share_recv = [next(take) for _ in range(9)]
    me = position()
    core = me["c"]
    partner = partner_of(me)
    own = me["x"] * 2 + core
    first = group_peers(me)[0]
    around = [moved(me, d, by) for d in "zy" for by in (1, -1)]
    half_up, half_down = up_ref.shape[-1] // PAIR, down_ref.shape[-1] // PAIR

    barrier = pltpu.get_barrier_semaphore()
    for device in [device for _, device in first] + around:
        pl.semaphore_signal(barrier, inc=1, device_id=device, device_id_type=MESH)
    pl.semaphore_wait(barrier, len(first) + len(around))

    sent = []

    def send(copy):
        copy.start()
        sent.append(copy)

    other = pl.ds(pl.multiple_of((1 - core) * half_down, LANES), half_down)
    core_copy = remote(down_ref.at[:, :, other], rows_down, core_send, core_recv, partner)
    send(core_copy)
    for t, (o, device) in enumerate(first):
        width = pl.ds(pl.multiple_of((o % PAIR) * half_up, LANES), half_up)
        send(remote(up_ref.at[:, :, width], rows_up.at[own], row_send.at[t], row_recv.at[own], device))

    def part(i, phase, owner, h=None, of=core):
        u = units[i]
        out, half = (out_up, half_up) if u.kind == "up" else (out_down, half_down)
        at = u.chunk(phase, owner, me, h)[0]
        at = at + (slice(None),) * (len(u.dims) + 1 - len(at))
        return out.at[(u.k,) + at + (pl.ds(pl.multiple_of(of * half + u.off, LANES), u.cols),)]

    def ring(i, phase, n):
        d = units[i].order[phase]
        by = 1 if n % PAIR == 0 else -1
        owner = me[d] if n < 4 else (me[d] - by) % RING
        ref = part(i, phase, owner, (0, 1, 1, 0, 0, 1)[n])
        s = (i * PHASES + phase) * SENDS + n
        return remote(ref, ref, ring_send.at[s], ring_recv.at[s], moved(me, d, by))

    def start_phase(i, phase):
        for n in range(4):
            send(ring(i, phase, n))

    shares = []

    def share(i, j, owner):
        phase = len(units[i].order) - 1
        mine, theirs = part(i, phase, owner), part(i, phase, owner, None, 1 - core)
        send(remote(mine, mine, share_send.at[i, j], share_recv.at[i, j], partner))
        shares.append(remote(theirs, theirs, share_send.at[i, j], share_recv.at[i, j], partner))

    rows_ready = [False]
    for i, s in events:
        u = units[i]
        last = len(u.order) - 1
        if s == 0:
            if u.kind == "down":
                if i == 0:
                    core_copy.wait_recv()
                low, high = down_ref[u.k, :, u.off:u.off + u.cols], down_ref[u.k, :, half_down + u.off:half_down + u.off + u.cols]
                mine = jnp.where(core == 0, low, high)
                theirs = rows_down[u.k, :, u.off:u.off + u.cols]
                block[i][...] = jnp.concatenate([jnp.where(core == 0, mine, theirs), jnp.where(core == 0, theirs, mine)], axis=0)
            else:
                if not rows_ready[0]:
                    rows_ready[0] = True
                    rows_up[own] = jnp.where(core == 0, up_ref[:, :, :half_up], up_ref[:, :, half_up:])
                    for o, device in first:
                        remote(rows_up.at[o], rows_up.at[o], row_send.at[0], row_recv.at[o], device).wait_recv()
                for p in range(8):
                    assembly[6 * p:6 * p + 6, :] = rows_up[p, u.k, :, u.off:u.off + u.cols].astype(F32)
                block[i][...] = assembly[...].astype(BF16)
            own_copy = pltpu.make_async_copy(block[i], part(i, 0, me[u.order[0]]), own_sem.at[i])
            own_copy.start()
            own_copy.wait()
            start_phase(i, 0)
        elif s % PAIR == 1:
            phase = (s - 1) // PAIR
            if phase == last:
                share(i, 0, me[u.order[last]])
            for n in (4, 5):
                d = u.order[phase]
                incoming = part(i, phase, (me[d] + (-1 if n == 4 else 1)) % RING, n - 4)
                remote(incoming, incoming, ring_send.at[0], ring_recv.at[(i * PHASES + phase) * SENDS + n - 4], moved(me, d, 1)).wait_recv()
                send(ring(i, phase, n))
        else:
            phase = s // PAIR - 1
            d = u.order[phase]
            for n in (PAIR, 3, 4, 5):
                step = {2: -1, 3: 1, 4: -2, 5: 2}[n]
                h = {2: 1, 3: 0, 4: 0, 5: 1}[n]
                incoming = part(i, phase, (me[d] + step) % RING, h)
                remote(incoming, incoming, ring_send.at[0], ring_recv.at[(i * PHASES + phase) * SENDS + n], moved(me, d, 1)).wait_recv()
                if phase == last and n == 3:
                    share(i, 1, (me[d] - 1) % RING)
                    share(i, 2, (me[d] + 1) % RING)
            if phase < last:
                start_phase(i, phase + 1)
            else:
                share(i, 3, (me[d] + 2) % RING)

    for copy in shares:
        copy.wait_recv()
    for copy in sent:
        copy.wait_send()


def gather_weights(block_up, block_down):
    up_cols, down_cols = block_up.shape[2], block_down.shape[2]
    units = column_groups(Gather, GATHER + GATHER_LATE, up_cols // PAIR, down_cols // PAIR)
    here = dict(x=0, y=0, z=0)
    phases = [[(d, half_bytes(u.chunk(p, 0, here, 0)[1], BF16)) for p, d in enumerate(u.order)] for u in units]
    events = serve_order((), [2.0 if u.kind == "down" else 6.0 for u in units], phases, 0, math.inf)[0]
    n = len(units)
    dma = pltpu.SemaphoreType.DMA
    scratch = [pltpu.VMEM((ROWS, u.cols), BF16) for u in units]
    scratch += [pltpu.VMEM((8, 2, 6, up_cols // PAIR), BF16), pltpu.VMEM((PAIR, HALF, down_cols // PAIR), BF16), pltpu.VMEM((ROWS, up_cols // 4), F32)]
    scratch += [dma((7,)), dma((8,)), dma, dma, dma((n * PHASES * SENDS,)), dma((n * PHASES * SENDS,)), dma((n,)), dma((n, 4)), dma((n, 4))]
    vmem = pl.BlockSpec(memory_space=pltpu.VMEM)
    out_up, out_down = pl.pallas_call(
        functools.partial(gather_kernel, units, events),
        out_shape=[jax.ShapeDtypeStruct((PAIR, RING, RING, ROWS, up_cols), BF16), jax.ShapeDtypeStruct((PAIR, RING, RING, RING, ROWS, down_cols), BF16)],
        in_specs=[vmem] * 2,
        out_specs=[pl.BlockSpec(memory_space=pl.ANY)] * 2,
        scratch_shapes=scratch,
        compiler_params=pltpu.CompilerParams(collective_id=1, has_side_effects=True, vmem_limit_bytes=HALF * 1024 * 1024),
        name="gather_weights",
    )(block_up, block_down)
    return out_up, out_down


def finish_weights_kernel(up, down, out_up, out_down, sems):
    copies = [pltpu.make_async_copy(src.at[k, z], dst.at[k, z], sems.at[i, k, z]) for i, (src, dst) in enumerate(((up, out_up), (down, out_down))) for k in range(PAIR) for z in range(RING)]
    for copy in copies:
        copy.start()
    for copy in copies:
        copy.wait()


def finish_state_kernel(*refs):
    n = len(refs) // 3
    into = [pltpu.make_async_copy(src, buf, refs[-1].at[i]) for i, (src, buf) in enumerate(zip(refs[:n], refs[PAIR * n:-1]))]
    back = [pltpu.make_async_copy(buf, dst, refs[-1].at[i]) for i, (buf, dst) in enumerate(zip(refs[PAIR * n:-1], refs[n:]))]
    for copy in into:
        copy.start()
    for one, other in zip(into, back):
        one.wait()
        other.start()
    for copy in back:
        copy.wait()


def finish(kernel, arrays, scratch, limit):
    any_space = pl.BlockSpec(memory_space=pl.ANY)
    return pl.pallas_call(
        kernel,
        out_shape=[jax.ShapeDtypeStruct(a.shape, a.dtype) for a in arrays],
        in_specs=[any_space] * len(arrays),
        out_specs=[any_space] * len(arrays),
        scratch_shapes=scratch,
        compiler_params=pltpu.CompilerParams(vmem_limit_bytes=limit),
    )(*arrays)


def solution(mesh):
    batch_rows = P("data", None)
    state_rows = P(None, "data", None)
    replicated = P()

    def device_step(act_in, grad_out, w_up, w_down, master_up, master_down, exp_avg_up, exp_avg_down, exp_sq_up, exp_sq_down, learn_rate, clip_norm):
        act_one, slope_one, hidden, act_three, slope_three = forward(act_in, w_up, w_down)
        tensors = (act_in, grad_out, hidden, act_one, act_three, slope_one, slope_three, w_up, w_down)
        outs = grad_update(tensors, (master_up, master_down), (exp_avg_up, exp_avg_down), (exp_sq_up, exp_sq_down), learn_rate, clip_norm)
        dma = pltpu.SemaphoreType.DMA
        small = [pltpu.VMEM(a.shape, F32) for a in outs[2:]]
        *state, norm = finish(finish_state_kernel, outs[2:], small + [dma((len(small),))], FULL_VMEM)
        new_w_up, new_w_down = finish(finish_weights_kernel, gather_weights(*outs[:2]), [dma((PAIR, PAIR, RING))], WEIGHT_LIMIT)
        state = [a.transpose(1, 0, 2) if i % PAIR == 0 else a for i, a in enumerate(state)]
        return (new_w_up.reshape(w_up.shape), new_w_down.reshape(w_down.shape), *state, norm[0, 0])

    return jax.shard_map(device_step, mesh=mesh, in_specs=(batch_rows, batch_rows, replicated, replicated, state_rows, state_rows, state_rows, state_rows, state_rows, state_rows, replicated, replicated), out_specs=(replicated, replicated, state_rows, state_rows, state_rows, state_rows, state_rows, state_rows, replicated), check_vma=False)
```
